256 devices in a mesh: parts: 2 (over z), seq: 128 (over x, y, core).
Axes of the slice: x: 8, y: 8, z: 2, core: 2. Of those that a mesh axis runs over, the one named last changes fastest.
The devices are a block of a 8x8x16 slice.
Arguments:
- token_ids: int32 [4, 4], P(None, 'parts'), parts along dimension 1, may hold values from 0 to 76031
- lengths: int32 [4], P('parts'), parts along dimension 0, may hold values from 24576 to 32768, as said below
- embed_table: bfloat16 [76032, 5120], P('seq'), may hold values from -6 to 6
- attn_gain: bfloat16 [5120], replicated, may hold values from 0.25 to 1.75
- w_qkv: bfloat16 [5120, 7168], P('seq'), may hold values from -0.3125 to 0.3125
- qkv_bias: float32 [7168], replicated, may hold values from -8 to 8
- cache_keys: bfloat16 [4, 32768, 1024], P('parts', 'seq'), parts along dimension 0, may hold values from -300 to 300
- cache_values: bfloat16 [4, 32768, 1024], P('parts', 'seq'), parts along dimension 0, may hold values from -6 to 6
- w_out: bfloat16 [5120, 5120], P(None, 'seq'), may hold values from -0.078125 to 0.078125
- mlp_gain: bfloat16 [5120], replicated, may hold values from 0.25 to 1.75
- w_gate: bfloat16 [5120, 16384], P(None, 'seq'), may hold values from -0.078125 to 0.078125
- w_up: bfloat16 [5120, 16384], P(None, 'seq'), may hold values from -0.078125 to 0.078125
- w_down: bfloat16 [16384, 5120], P('seq'), may hold values from -0.1875 to 0.1875
Outputs:
- attended: bfloat16 [4, 4, 5120], P(None, 'parts'), parts along dimension 1
- layer_out: bfloat16 [4, 4, 5120], P(None, 'parts', 'seq'), parts along dimension 1
The draws below stay inside these ranges and needn't reach their ends.
There are 2 independent parts, one for each index of `parts`. The reference program is written for one: setup_inputs(seed, part) draws one part's arguments, and reference() takes and returns one part's arrays. A program takes and returns all parts, laid end to end along the dimension named above; an argument that names none is the same for every part. Nothing has to cross between parts.
Inputs may be any that keep to these rules, and one draw needn't show every extreme that they name: Cache positions lengths[b] and later are unused; the first prompt fills the whole cache of 32768 positions.
All inputs are finite; a program needn't handle non-finite values.
Results may differ from the reference program's by a relative error of at most 0.017.
The reference program's roundings to bfloat16 on the way (of `normed`, `joint`, `normed_mid` and `hidden`) count: a program that leaves them out, or rounds other values in their place, can miss the bound.
Values may be sent and summed in bfloat16 or wider, within the bound.
A program may use at most 128 MiB of HBM per device.

```python
import jax
import jax.numpy as jnp
from jax import lax

D = 5120
HEADS = 40
KV_HEADS = 8
HEAD_DIM = 128
FF = 16384
VOCAB = 76032
CTX = 32768
STEPS = 4
SEQS = 2
QD = 5120
KVD = 1024
QKV = 7168


def draw_lengths(key, part):
    drawn = jax.random.randint(jax.random.fold_in(key, 3), (SEQS,), CTX - CTX // 4, CTX + 1, dtype=jnp.int32)
    return drawn.at[0].set(CTX)


def draw_qkv_bias(key, part):
    key_one, key_two, key_three, key_four = jax.random.split(jax.random.fold_in(key, 11), 4)
    direction = jax.random.normal(key_one, (KV_HEADS, HEAD_DIM), jnp.float32)
    strength = jax.random.uniform(key_two, (KV_HEADS, 1), jnp.float32, 1.05, 1.3)
    aligned = direction * strength
    query_noise = 0.5 * jax.random.normal(key_three, (KV_HEADS, HEADS // KV_HEADS, HEAD_DIM), jnp.float32)
    query_part = (aligned[:, None, :] + query_noise).reshape(HEADS * HEAD_DIM)
    key_part = aligned.reshape(KV_HEADS * HEAD_DIM)
    value_part = 0.5 * jax.random.normal(key_four, (KV_HEADS * HEAD_DIM,), jnp.float32)
    joined = jnp.concatenate([query_part, key_part, value_part])
    return jnp.clip(joined, -8.0, 8.0)


def draw_cache_keys(key, part):
    key_one = jax.random.fold_in(jax.random.fold_in(key, 17), 0)
    base = 2.2 * jax.random.normal(key_one, (SEQS, CTX, KV_HEADS, HEAD_DIM), jnp.float32)
    return jnp.clip(base, -300.0, 300.0).reshape(SEQS, CTX, KV_HEADS * HEAD_DIM).astype(jnp.bfloat16)


def touch_ends(entries, key, low, largest):
    dims = entries.shape
    index_at = [jax.random.randint(jax.random.fold_in(key, axis), (), 0, dims[axis]) for axis in range(len(dims))]
    entries = entries.at[tuple(index_at)].set(low)
    longest = dims.index(max(dims))
    index_at[longest] = (index_at[longest] + 1) % dims[longest]
    return entries.at[tuple(index_at)].set(largest)


def spiked(values, rng, source, target, parts, factor):
    def block_of(dim):
        return (jnp.arange(values.shape[dim]) // (values.shape[dim] // parts)).reshape((-1,) + (1,) * (values.ndim - 1 - dim))

    first = jax.random.permutation(rng, parts)[block_of(target)]
    far = (block_of(target) + parts // 2) % parts
    return jnp.where((block_of(source) == first) | (block_of(source) == far), factor * values, values)


def level_of(rng, shape, shards, smallest, top_value):
    level, own = 1.0, jax.random.fold_in(rng, 6)
    for dim, parts in shards:
        steps = jnp.exp(jax.random.uniform(jax.random.fold_in(own, dim), (parts,), jnp.float32, smallest / len(shards), top_value / len(shards)))
        level = level * jnp.repeat(steps, shape[dim] // parts).reshape([-1 if axis == dim else 1 for axis in range(len(shape))])
    return level


def gaussian(key, shape, spread, most, pieces=(), held_as=jnp.bfloat16):
    values = jax.random.normal(key, shape, jnp.float32) * spread
    if len(pieces) > 0:
        values = level_of(key, shape, pieces, -0.22, 0.18) * values
    return jnp.clip(values, min=-most, max=most).astype(held_as)


def heavy_noise(own_key, shape, spread, most, shards, heavy, held_as=jnp.bfloat16):
    entries = spread * jax.random.normal(own_key, shape, jnp.float32)
    if shards:
        entries = entries * level_of(own_key, shape, shards, -0.22, 0.18)
    return jnp.clip(spiked(entries, jax.random.fold_in(own_key, 3), *heavy), -most, most).astype(held_as)


def setup_inputs(seed: int = 0, part: int = 0) -> dict:
    streams_of = jax.random.split(jax.random.key(seed), 14)
    part_keys = jax.random.split(jax.random.fold_in(streams_of[13], part), 14)
    token_ids = touch_ends(jax.random.randint(part_keys[0], (STEPS, SEQS), 0, VOCAB), jax.random.fold_in(part_keys[0], 1), 0, VOCAB - 1).astype(jnp.int32)
    lengths = draw_lengths(jax.random.fold_in(jax.random.fold_in(streams_of[13], part), 71), part)
    embed_table = gaussian(streams_of[2], (VOCAB, D), 0.5, 6.0, ((0, 128),))
    attn_gain = jnp.clip(1.0 + 0.15 * jax.random.normal(streams_of[3], (D,), jnp.float32), 0.25, 1.75).astype(jnp.bfloat16)
    w_qkv = heavy_noise(streams_of[4], (D, QKV), D ** -0.5, 0.3125, ((0, 128),), (0, 1, 128, 5.5))
    qkv_bias = draw_qkv_bias(jax.random.fold_in(streams_of[13], 71), part)
    cache_keys = draw_cache_keys(jax.random.fold_in(jax.random.fold_in(streams_of[13], part), 71), part)
    cache_values = gaussian(part_keys[7], (SEQS, CTX, KVD), 1.0, 6.0, ((1, 128),))
    w_out = gaussian(streams_of[8], (QD, D), QD ** -0.5, 0.078125, ((1, 128),))
    mlp_gain = jnp.clip(1.0 + 0.15 * jax.random.normal(streams_of[9], (D,), jnp.float32), 0.25, 1.75).astype(jnp.bfloat16)
    w_gate = gaussian(streams_of[10], (D, FF), D ** -0.5, 0.078125, ((1, 128),))
    w_up = gaussian(streams_of[11], (D, FF), D ** -0.5, 0.078125, ((1, 128),))
    w_down = heavy_noise(streams_of[12], (FF, D), FF ** -0.5, 0.1875, ((0, 128),), (0, 1, 128, 5.5))
    return {"token_ids": token_ids, "lengths": lengths, "embed_table": embed_table, "attn_gain": attn_gain, "w_qkv": w_qkv, "qkv_bias": qkv_bias, "cache_keys": cache_keys, "cache_values": cache_values, "w_out": w_out, "mlp_gain": mlp_gain, "w_gate": w_gate, "w_up": w_up, "w_down": w_down}


NORM_EPS = 1e-06
ROPE_BASE = 1000000.0
MASKED = -1e+30

def rms_normalize(rows, gain):
    mean_square = lax.optimization_barrier(jnp.mean(rows * rows, axis=-1, keepdims=True))
    return (rows * lax.rsqrt(mean_square + NORM_EPS) * gain.astype(jnp.float32)).astype(jnp.bfloat16)

def rotate(vectors, positions):
    half_dim = vectors.shape[-1] // 2
    frequency = ROPE_BASE ** (-2.0 * jnp.arange(half_dim, dtype=jnp.float32) / vectors.shape[-1])
    angles = positions.astype(jnp.float32)[..., None, None] * frequency
    cosine = jnp.cos(angles)
    sine_part = jnp.sin(angles)
    widened = vectors.astype(jnp.float32)
    first_half = widened[..., :half_dim]
    second = widened[..., half_dim:]
    joined = jnp.concatenate([first_half * cosine - second * sine_part, second * cosine + first_half * sine_part], axis=-1)
    return joined.astype(jnp.bfloat16)

def attend_one(query_rows, key_rows, value_rows, cached_keys, cached_values, length):
    all_keys = jnp.concatenate([cached_keys.reshape(CTX, KV_HEADS, HEAD_DIM), key_rows], axis=0).astype(jnp.float32)
    all_values = jnp.concatenate([cached_values.reshape(CTX, KV_HEADS, HEAD_DIM), value_rows], axis=0).astype(jnp.float32)
    grouped = query_rows.reshape(STEPS, KV_HEADS, HEADS // KV_HEADS, HEAD_DIM).astype(jnp.float32)
    scores = jnp.einsum('skgd,pkd->kgsp', grouped, all_keys) * HEAD_DIM ** (-0.5)
    places = jnp.arange(CTX + STEPS, dtype=jnp.int32)
    step_index = jnp.arange(STEPS, dtype=jnp.int32)
    cache_valid = places[None, :] < length
    new_valid = places[None, :] - CTX <= step_index[:, None]
    valid = jnp.where(places[None, :] < CTX, cache_valid, new_valid)
    masked = jnp.where(valid, scores, MASKED)
    top_score = lax.optimization_barrier(jnp.max(masked, axis=-1, keepdims=True))
    weights = jnp.where(valid, jnp.exp(masked - top_score), 0.0)
    total = lax.optimization_barrier(jnp.sum(weights, axis=-1))
    rounded = lax.optimization_barrier(weights.astype(jnp.bfloat16)).astype(jnp.float32)
    summed = jnp.einsum('kgsp,pkd->kgsd', rounded, all_values)
    result = summed / total[..., None]
    result = jnp.transpose(result, (2, 0, 1, 3))
    return result.reshape(STEPS, HEADS * HEAD_DIM).astype(jnp.bfloat16)

def reference(token_ids, lengths, embed_table, attn_gain, w_qkv, qkv_bias, cache_keys, cache_values, w_out, mlp_gain, w_gate, w_up, w_down):
    query_width = HEADS * HEAD_DIM
    key_width = KV_HEADS * HEAD_DIM
    stream = embed_table[token_ids].astype(jnp.float32)
    normed = rms_normalize(stream, attn_gain)
    joint = jnp.dot(normed.reshape(-1, D), w_qkv, preferred_element_type=jnp.float32) + qkv_bias.astype(jnp.float32)
    joint = joint.astype(jnp.bfloat16).reshape(STEPS, SEQS, -1)
    query_part = joint[..., :query_width].reshape(STEPS, SEQS, HEADS, HEAD_DIM)
    key_part = joint[..., query_width:query_width + key_width].reshape(STEPS, SEQS, KV_HEADS, HEAD_DIM)
    value_part = joint[..., query_width + key_width:].reshape(STEPS, SEQS, KV_HEADS, HEAD_DIM)
    positions = lengths[None, :] + jnp.arange(STEPS, dtype=jnp.int32)[:, None]
    queries = rotate(query_part, positions)
    new_keys = rotate(key_part, positions)
    outputs = []
    for seq_index in range(SEQS):
        outputs.append(attend_one(queries[:, seq_index], new_keys[:, seq_index], value_part[:, seq_index], cache_keys[seq_index], cache_values[seq_index], lengths[seq_index]))
    attended = jnp.stack(outputs, axis=1)
    projected = jnp.dot(attended.reshape(-1, query_width), w_out, preferred_element_type=jnp.float32)
    mid = stream + projected.reshape(STEPS, SEQS, D)
    normed_mid = rms_normalize(mid, mlp_gain).reshape(-1, D)
    gate = jnp.dot(normed_mid, w_gate, preferred_element_type=jnp.float32)
    upper = jnp.dot(normed_mid, w_up, preferred_element_type=jnp.float32)
    hidden = (jax.nn.silu(gate) * upper).astype(jnp.bfloat16)
    down = jnp.dot(hidden, w_down, preferred_element_type=jnp.float32).reshape(STEPS, SEQS, D)
    layer_out = (mid + down).astype(jnp.bfloat16)
    return (attended, layer_out)
```

```python
import functools
import math

import jax
import jax.numpy as jnp
import numpy as np
from jax import lax
from jax.experimental import pallas as pl
from jax.experimental.pallas import tpu as pltpu
from jax.sharding import PartitionSpec as P

HEADS = 40
KV_HEADS = 8
HEAD_DIM = 128
NORM_EPS = 1e-06
ROPE_BASE = 1000000.0
MASKED = -1e30

ROWS = 8
LANES = 128
XS, YS, CORES = 8, 8, 2
PLANE = YS * CORES
CHIPS = XS * YS
GROUP = CHIPS * CORES
JOINT_HEADS = HEADS + 2 * KV_HEADS
HALF_JOINT = JOINT_HEADS // CORES
HALF_HEADS = HEADS // CORES
MESH = pl.DeviceIdType.MESH
F32, BF16 = jnp.float32, jnp.bfloat16


def chip_of(i, count):
    return (CHIPS * i) // count


def tile_of(chip, count):
    i = lax.div(count * chip + CHIPS - 1, CHIPS)
    ok = jnp.logical_and(i < count, lax.div(CHIPS * i, count) == chip)
    return jnp.minimum(i, count - 1), ok


def lanes_of(n):
    return pl.ds(pl.multiple_of(n * LANES, LANES), LANES)


def send(src, dst, send_sem, recv_sem, device):
    copy = pltpu.make_async_remote_copy(
        src_ref=src,
        dst_ref=dst,
        send_sem=send_sem,
        recv_sem=recv_sem,
        device_id={"seq": device},
        device_id_type=MESH,
    )
    copy.start()


def wait_bytes(ref, sem):
    pltpu.make_async_copy(ref, ref, sem).wait()


def cut_pieces(tiles, width, count):
    lane = lax.broadcasted_iota(jnp.int32, (ROWS, LANES), 1)
    pieces = []
    for j in range(count):
        t, off = divmod(width * j, LANES)
        piece = tiles[t] if off == 0 else pltpu.roll(tiles[t], LANES - off, 1)
        if off + width > LANES:
            rest = pltpu.roll(tiles[t + 1], LANES - off, 1)
            piece = jnp.where(lane < LANES - off, piece, rest)
        pieces.append(piece)
    return pieces


def join_pieces(pieces, width, tiles):
    lane = lax.broadcasted_iota(jnp.int32, (ROWS, LANES), 1)
    out = [None] * tiles

    def put(t, value):
        out[t] = value if out[t] is None else out[t] + value

    for j, piece in enumerate(pieces):
        t, off = divmod(width * j, LANES)
        moved = piece if off == 0 else pltpu.roll(piece, off, 1)
        if off + width > LANES:
            put(t, jnp.where(lane >= off, moved, 0.0))
            put(t + 1, jnp.where(lane < off, moved, 0.0))
        else:
            put(t, moved)
    return out


def kernel(
    ids_ref, len_ref, freq_ref, table_hbm, gain_ref, wqkv_hbm, bias_ref, keys_hbm, values_hbm,
    wout_hbm, mgain_ref, wgate_hbm, wup_hbm, wdown_hbm,
    att_ref, lay_ref,
    table, wqkv, keys, values, wout, wgate, wup, wdown,
    rows_f, n1s, n1r, t1s, t1r, n2s, n2r, t2s, t2r, cosr, sinr,
    part, bx, bs, br, jflat,
    ob, cx, cs, cr, aflat, tmp, ds_, dx, mb, nflat,
    es, er, e2s, e2r, dummy,
    tsem, wsem, ssem, rsem,
):
    me = lax.axis_index("seq")
    x = lax.div(me, PLANE)
    j0 = lax.rem(me, PLANE)
    chip = lax.div(me, CORES)
    c = lax.rem(me, CORES)
    other = me + 1 - 2 * c
    width = lay_ref.shape[1]
    block = PLANE * width
    tiles = block // LANES
    vocab_rows = table.shape[0]

    x_peers = [(k, lax.rem(x + k, XS)) for k in range(1, XS)]
    j_peers = [(k, lax.rem(j0 + k, PLANE)) for k in range(1, PLANE)]

    loads = []
    for k in range(XS):
        at = pl.ds(k * block, block)
        loads.append(pltpu.make_async_copy(table_hbm.at[:, at], table.at[:, at], tsem.at[k]))
        loads[-1].start()
    barrier = pltpu.get_barrier_semaphore()
    for _, p in x_peers:
        pl.semaphore_signal(barrier, inc=1, device_id={"seq": p * PLANE + j0}, device_id_type=MESH)
    for _, p in j_peers:
        pl.semaphore_signal(barrier, inc=1, device_id={"seq": x * PLANE + p}, device_id_type=MESH)
    weights = [
        pltpu.make_async_copy(src, dst, wsem.at[k])
        for k, (src, dst) in enumerate(
            [(wqkv_hbm, wqkv), (keys_hbm, keys), (values_hbm, values), (wout_hbm, wout),
             (wgate_hbm, wgate), (wup_hbm, wup), (wdown_hbm, wdown)]
        )
    ]
    for w in weights:
        w.start()

    lane = lax.broadcasted_iota(jnp.int32, (ROWS, LANES), 1)
    row = lax.broadcasted_iota(jnp.int32, (ROWS, LANES), 0)
    prompts = len_ref.shape[0]

    local = jnp.full((ROWS, vocab_rows), -1, jnp.int32)
    vrow = lax.broadcasted_iota(jnp.int32, (ROWS, vocab_rows), 0)
    vcol = lax.broadcasted_iota(jnp.int32, (ROWS, vocab_rows), 1)
    for r in range(ROWS):
        local = jnp.where(vrow == r, ids_ref[r % prompts, r // prompts] - me * vocab_rows, local)
    chosen = jnp.where(local == vcol, 1.0, 0.0).astype(BF16)
    square = jnp.zeros((ROWS, LANES), F32)
    for k in range(XS):
        loads[k].wait()
        found = jnp.dot(chosen, table[:, k * block : (k + 1) * block], preferred_element_type=F32)
        rows_f[:, k * block : (k + 1) * block] = found
        t1s[k] = found.astype(BF16)
        for t in range(tiles):
            v = found[:, t * LANES : (t + 1) * LANES]
            square = square + v * v
    scale = lax.rsqrt(jnp.sum(square, axis=-1, keepdims=True) / (XS * block) + NORM_EPS)
    gain = gain_ref[...].astype(F32)
    for k in range(XS):
        for t in range(tiles):
            g = k * tiles + t
            v = rows_f[:, g * LANES : (g + 1) * LANES] * scale * gain[g : g + 1, :]
            n1s[k, :, t * LANES : (t + 1) * LANES] = v.astype(BF16)

    pl.semaphore_wait(barrier, XS + PLANE - 2)

    for k, p in x_peers:
        send(n1s.at[p], n1r.at[k - 1], ssem.at[0], rsem.at[0], p * PLANE + j0)
    for k, p in x_peers:
        send(t1s.at[p], t1r.at[k - 1], ssem.at[1], rsem.at[1], p * PLANE + j0)

    place = jnp.zeros((ROWS, LANES), jnp.int32)
    for r in range(ROWS):
        place = jnp.where(row == r, len_ref[r % prompts] + r // prompts, place)
    angle = place.astype(F32) * freq_ref[...]
    cosr[...] = jnp.cos(angle)
    sine = jnp.sin(angle)
    sinr[...] = jnp.where(lane < HEAD_DIM // 2, -sine, sine)

    def gather_block(own, got):
        total = own[x].astype(F32)
        for k in range(XS - 1):
            total = total + got[k].astype(F32)
        return [total[:, t * LANES : (t + 1) * LANES] for t in range(tiles)]

    wait_bytes(n1r, rsem.at[0])
    for j, piece in enumerate(cut_pieces(gather_block(n1s, n1r), width, PLANE)):
        n2s[j] = piece
    for k, p in j_peers:
        send(n2s.at[p], n2r.at[k - 1], ssem.at[2], rsem.at[2], x * PLANE + p)
    wait_bytes(t1r, rsem.at[1])
    for j, piece in enumerate(cut_pieces(gather_block(t1s, t1r), width, PLANE)):
        t2s[j] = piece
    for k, p in j_peers:
        send(t2s.at[p], t2r.at[k - 1], ssem.at[3], rsem.at[3], x * PLANE + p)
    weights[0].wait()
    wait_bytes(n2r, rsem.at[2])
    normed = n2s[j0] + jnp.sum(n2r[...], axis=0)
    normed = normed[:, :width].astype(BF16)

    per = JOINT_HEADS // XS
    for k in range(XS):
        got = jnp.dot(
            normed, wqkv[:, k * per * LANES : (k + 1) * per * LANES], preferred_element_type=F32
        )
        for t in range(per):
            part[k * per + t] = got[:, t * LANES : (t + 1) * LANES]
    send(part.at[pl.ds(HALF_JOINT * (1 - c), HALF_JOINT)], bx, ssem.at[4], rsem.at[4], other)
    wait_bytes(bx, rsem.at[4])
    bs[...] = part[pl.ds(HALF_JOINT * c, HALF_JOINT)] + bx[...]
    for i in range(HALF_JOINT):
        p = chip_of(i, HALF_JOINT)

        @pl.when(chip != p)
        def _(i=i, p=p):
            slot = lax.rem(chip - p + CHIPS, CHIPS) - 1
            send(bs.at[i], br.at[slot], ssem.at[5], rsem.at[5], p * CORES + c)

    ib, b_on = tile_of(chip, HALF_JOINT)
    hb = HALF_JOINT * c + ib

    @pl.when(b_on)
    def _():
        wait_bytes(br, rsem.at[5])
        total = bs[ib] + jnp.sum(br[...], axis=0) + bias_ref[pl.ds(hb, 1), :]
        joint = total.astype(BF16).astype(F32)
        turned = joint * cosr[...] + pltpu.roll(joint, HEAD_DIM // 2, 1) * sinr[...]
        turn = jnp.where(hb < HEADS + KV_HEADS, 1.0, 0.0)
        jflat[:, lanes_of(hb)] = jnp.where(turn > 0.5, turned, joint).astype(BF16)

        @pl.loop(1, GROUP)
        def _(k):
            at = jflat.at[:, lanes_of(hb)]
            send(at, at, ssem.at[6], rsem.at[6], lax.rem(me + k, GROUP))

        wait_bytes(jflat.at[:, : (JOINT_HEADS - 1) * LANES], rsem.at[6])

    @pl.when(jnp.logical_not(b_on))
    def _():
        wait_bytes(jflat, rsem.at[6])

    weights[1].wait()
    weights[2].wait()
    group = HEADS // KV_HEADS
    span = keys.shape[1]
    lines = group * ROWS
    wide_row = lax.broadcasted_iota(jnp.int32, (lines, span), 0)
    even = lax.rem(wide_row, prompts) == 0
    where = me * span + lax.broadcasted_iota(jnp.int32, (lines, span), 1)
    valid = where < jnp.where(even, len_ref[0], len_ref[1])
    score_scale = 1.0 / math.sqrt(HEAD_DIM)
    nt = (((1,), (1,)), ((), ()))
    for k in range(KV_HEADS):
        at = slice(k * LANES, (k + 1) * LANES)
        query = jnp.concatenate(
            [
                jflat[:, h * LANES : (h + 1) * LANES].astype(F32)
                for h in range(k * group, (k + 1) * group)
            ],
            axis=0,
        ).astype(BF16)
        score = [
            lax.dot_general(query, keys[b, :, at], nt, preferred_element_type=F32)
            for b in range(prompts)
        ]
        score = jnp.where(valid, jnp.where(even, score[0], score[1]) * score_scale, MASKED)
        top = jnp.max(score, axis=-1, keepdims=True)
        weight = jnp.where(valid, jnp.exp(score - top), 0.0)
        total = jnp.sum(weight, axis=-1, keepdims=True)
        summed = jnp.dot(
            jnp.where(even, weight, 0.0).astype(BF16), values[0, :, at], preferred_element_type=F32
        ) + jnp.dot(
            jnp.where(even, 0.0, weight).astype(BF16), values[1, :, at], preferred_element_type=F32
        )
        top = jnp.broadcast_to(top, (lines, LANES))
        total = jnp.broadcast_to(total, (lines, LANES))
        for g in range(group):
            h = k * group + g
            ob[h, 0] = summed[g * ROWS : (g + 1) * ROWS]
            ob[h, 1] = top[g * ROWS : (g + 1) * ROWS]
            ob[h, 2] = total[g * ROWS : (g + 1) * ROWS]

    send(ob.at[pl.ds(HALF_HEADS * (1 - c), HALF_HEADS)], cx, ssem.at[7], rsem.at[7], other)
    wait_bytes(cx, rsem.at[7])
    for i in range(HALF_HEADS):
        h = HALF_HEADS * c + i
        top_a, top_b = ob[h, 1], cx[i, 1]
        top = jnp.maximum(top_a, top_b)
        scale_a, scale_b = jnp.exp(top_a - top), jnp.exp(top_b - top)
        cs[i, 0] = ob[h, 0] * scale_a + cx[i, 0] * scale_b
        cs[i, 1] = jnp.where(lane < LANES // 2, top, ob[h, 2] * scale_a + cx[i, 2] * scale_b)
    for i in range(HALF_HEADS):
        p = chip_of(i, HALF_HEADS)

        @pl.when(chip != p)
        def _(i=i, p=p):
            slot = lax.rem(chip - p + CHIPS, CHIPS) - 1
            send(cs.at[i], cr.at[slot], ssem.at[8], rsem.at[8], p * CORES + c)

    ic, c_on = tile_of(chip, HALF_HEADS)
    hc = HALF_HEADS * c + ic

    @pl.when(c_on)
    def _():
        kv = lax.div(hc, group)
        query = jflat[:, lanes_of(hc)]
        new_key = jflat[:, lanes_of(HEADS + kv)]
        new_value = jflat[:, lanes_of(HEADS + KV_HEADS + kv)]
        small_r = lax.broadcasted_iota(jnp.int32, (ROWS, ROWS), 0)
        small_c = lax.broadcasted_iota(jnp.int32, (ROWS, ROWS), 1)
        seen = jnp.logical_and(
            small_c <= small_r, lax.rem(small_c, prompts) == lax.rem(small_r, prompts)
        )
        score = lax.dot_general(query, new_key, nt, preferred_element_type=F32) * score_scale
        score = jnp.where(seen, score, MASKED)
        top = jnp.max(score, axis=-1, keepdims=True)
        weight = jnp.where(seen, jnp.exp(score - top), 0.0)
        total = jnp.sum(weight, axis=-1, keepdims=True)
        new_sum = jnp.dot(weight.astype(BF16), new_value, preferred_element_type=F32)
        low = lane < LANES // 2
        new_stat = jnp.where(
            low, jnp.broadcast_to(top, (ROWS, LANES)), jnp.broadcast_to(total, (ROWS, LANES))
        )
        wait_bytes(cr, rsem.at[8])
        stats = [new_stat, cs[ic, 1]] + [cr[s, 1] for s in range(CHIPS - 1)]
        sums = [new_sum, cs[ic, 0]] + [cr[s, 0] for s in range(CHIPS - 1)]
        best = functools.reduce(jnp.maximum, stats)
        acc = jnp.zeros((ROWS, LANES), F32)
        den = jnp.zeros((ROWS, LANES), F32)
        for stat, value in zip(stats, sums):
            scale = jnp.exp(stat - best)
            scale = jnp.where(low, scale, pltpu.roll(scale, LANES // 2, 1))
            acc = acc + value * scale
            den = den + stat * scale
        den = jnp.where(low, pltpu.roll(den, LANES // 2, 1), den)
        aflat[:, lanes_of(hc)] = (acc / den).astype(BF16)

        @pl.loop(1, GROUP)
        def _(k):
            at = aflat.at[:, lanes_of(hc)]
            send(at, at, ssem.at[9], rsem.at[9], lax.rem(me + k, GROUP))

        wait_bytes(aflat.at[:, : (HEADS - 1) * LANES], rsem.at[9])

    @pl.when(jnp.logical_not(c_on))
    def _():
        wait_bytes(aflat, rsem.at[9])

    weights[3].wait()
    attended = aflat[...]
    tmp[...] = jnp.zeros((ROWS, LANES), F32)
    tmp[:, :width] = lax.dot_general(attended, wout[...], nt, preferred_element_type=F32)
    wait_bytes(t2r, rsem.at[3])
    stream = t2s[j0] + jnp.sum(t2r[...], axis=0)
    mid = jnp.where(lane < width, tmp[...] + stream, 0.0)
    mine = jnp.where(lax.rem(row * 0 + c, CORES) == 0, mid, pltpu.roll(mid, width, 1))
    ds_[...] = mine
    send(ds_, dx, ssem.at[10], rsem.at[10], other)
    wait_bytes(dx, rsem.at[10])
    mb[chip] = mine + dx[...]

    @pl.loop(1, CHIPS)
    def _(k):
        to = lax.rem(chip + k, CHIPS)
        send(mb.at[chip], mb.at[chip], ssem.at[11], rsem.at[11], to * CORES + c)

    att_ref[...] = attended
    weights[4].wait()
    weights[5].wait()
    weights[6].wait()
    wait_bytes(mb.at[pl.ds(0, CHIPS - 1)], rsem.at[11])
    mids = join_pieces([mb[p] for p in range(CHIPS)], CORES * width, XS * tiles)
    square = jnp.zeros((ROWS, LANES), F32)
    for v in mids:
        square = square + v * v
    scale = lax.rsqrt(jnp.sum(square, axis=-1, keepdims=True) / (XS * block) + NORM_EPS)
    gain = mgain_ref[...].astype(F32)
    for g, v in enumerate(mids):
        nflat[:, g * LANES : (g + 1) * LANES] = (v * scale * gain[g : g + 1, :]).astype(BF16)
    normed_mid = nflat[...]
    gate = jnp.dot(normed_mid, wgate[...], preferred_element_type=F32)
    upper = jnp.dot(normed_mid, wup[...], preferred_element_type=F32)
    hidden = (gate / (1.0 + jnp.exp(-gate)) * upper).astype(BF16)
    for k in range(XS):
        es[k] = jnp.dot(
            hidden, wdown[:, k * block : (k + 1) * block], preferred_element_type=F32
        )
    for k, p in x_peers:
        send(es.at[p], er.at[k - 1], ssem.at[12], rsem.at[12], p * PLANE + j0)
    wait_bytes(er, rsem.at[12])
    for j, piece in enumerate(cut_pieces(gather_block(es, er), width, PLANE)):
        e2s[j] = piece
    for k, p in j_peers:
        send(e2s.at[p], e2r.at[k - 1], ssem.at[13], rsem.at[13], x * PLANE + p)
    wait_bytes(e2r, rsem.at[13])
    final = mid + e2s[j0] + jnp.sum(e2r[...], axis=0)
    lay_ref[...] = final[:, :width].astype(BF16)

    for sem, ref in (
        (0, n1r), (1, t1r), (2, n2r), (3, t2r), (4, bx), (7, cx), (10, dx), (12, er), (13, e2r),
    ):
        wait_bytes(ref, ssem.at[sem])
    wait_bytes(mb.at[pl.ds(0, CHIPS - 1)], ssem.at[11])
    @pl.when(b_on)
    def _():
        wait_bytes(bs.at[pl.ds(0, HALF_JOINT - 1)], ssem.at[5])
        wait_bytes(dummy, ssem.at[6])

    @pl.when(jnp.logical_not(b_on))
    def _():
        wait_bytes(bs, ssem.at[5])

    @pl.when(c_on)
    def _():
        wait_bytes(cs.at[pl.ds(0, HALF_HEADS - 1)], ssem.at[8])
        wait_bytes(dummy, ssem.at[9])

    @pl.when(jnp.logical_not(c_on))
    def _():
        wait_bytes(cs, ssem.at[8])


def body(
    token_ids, lengths, embed_table, attn_gain, w_qkv, qkv_bias, cache_keys, cache_values, w_out,
    mlp_gain, w_gate, w_up, w_down,
):
    steps, prompts = token_ids.shape
    vocab_rows, model = embed_table.shape
    width = w_out.shape[1]
    block = PLANE * width
    half = HEAD_DIM // 2
    frequency = np.float32(ROPE_BASE) ** (
        np.float32(-2.0) * np.arange(half, dtype=np.float32) / np.float32(HEAD_DIM)
    )
    frequency = jnp.asarray(np.tile(np.concatenate([frequency, frequency]), (ROWS, 1)), F32)
    vmem = pl.BlockSpec(memory_space=pltpu.VMEM)
    smem = pl.BlockSpec(memory_space=pltpu.SMEM)
    hbm = pl.BlockSpec(memory_space=pl.ANY)
    w_out_t = w_out.T

    def like(a):
        return pltpu.VMEM(a.shape, a.dtype)

    def tile(*lead, dtype=F32):
        return pltpu.VMEM((*lead, ROWS, LANES), dtype)

    def wide(*lead, dtype):
        return pltpu.VMEM((*lead, ROWS, block), dtype)

    attended, layer_out = pl.pallas_call(
        kernel,
        out_shape=(
            jax.ShapeDtypeStruct((ROWS, HEADS * HEAD_DIM), BF16),
            jax.ShapeDtypeStruct((ROWS, width), BF16),
        ),
        in_specs=[smem, smem, vmem, hbm, vmem, hbm, vmem, hbm, hbm, hbm, vmem, hbm, hbm, hbm],
        out_specs=(vmem, vmem),
        scratch_shapes=[
            like(embed_table), like(w_qkv), like(cache_keys), like(cache_values), like(w_out_t),
            like(w_gate), like(w_up), like(w_down),
            pltpu.VMEM((ROWS, model), F32),
            wide(XS, dtype=BF16), wide(XS - 1, dtype=BF16),
            wide(XS, dtype=BF16), wide(XS - 1, dtype=BF16),
            tile(PLANE), tile(PLANE - 1), tile(PLANE), tile(PLANE - 1), tile(), tile(),
            tile(JOINT_HEADS), tile(HALF_JOINT), tile(HALF_JOINT), tile(CHIPS - 1),
            pltpu.VMEM((ROWS, JOINT_HEADS * LANES), BF16),
            tile(HEADS, 3), tile(HALF_HEADS, 3), tile(HALF_HEADS, 2), tile(CHIPS - 1, 2),
            pltpu.VMEM((ROWS, HEADS * LANES), BF16),
            tile(), tile(), tile(), tile(CHIPS),
            pltpu.VMEM((ROWS, model), BF16),
            wide(XS, dtype=F32), wide(XS - 1, dtype=F32), tile(PLANE), tile(PLANE - 1),
            tile(GROUP - 1, dtype=BF16),
            pltpu.SemaphoreType.DMA((XS,)),
            pltpu.SemaphoreType.DMA((7,)),
            pltpu.SemaphoreType.DMA((14,)),
            pltpu.SemaphoreType.DMA((14,)),
        ],
        compiler_params=pltpu.CompilerParams(
            collective_id=0, has_side_effects=True, vmem_limit_bytes=60 * 2**20
        ),
        name="layer",
    )(
        token_ids.T, lengths, frequency, embed_table, attn_gain.reshape(-1, LANES), w_qkv,
        qkv_bias.reshape(-1, LANES), cache_keys, cache_values, w_out_t,
        mlp_gain.reshape(-1, LANES), w_gate, w_up, w_down,
    )
    return (
        attended.reshape(steps, prompts, -1),
        layer_out.reshape(steps, prompts, width),
    )


def solution(mesh):
    return jax.shard_map(
        body,
        mesh=mesh,
        in_specs=(
            P(None, "parts"), P("parts"), P("seq", None), P(), P("seq", None), P(),
            P("parts", "seq", None), P("parts", "seq", None), P(None, "seq"), P(),
            P(None, "seq"), P(None, "seq"), P("seq", None),
        ),
        out_specs=(P(None, "parts", None), P(None, "parts", "seq")),
        check_vma=False,
    )
```

```python
import functools
import math

import jax
import jax.numpy as jnp
import numpy as np
from jax import lax
from jax.experimental import pallas as pl
from jax.experimental.pallas import tpu as pltpu
from jax.sharding import PartitionSpec as P

HEADS = 40
KV_HEADS = 8
HEAD_DIM = 128
NORM_EPS = 1e-06
ROPE_BASE = 1000000.0
MASKED = -1e30

ROWS = 8
LANES = 128
XS, YS, CORES = 8, 8, 2
PLANE = YS * CORES
CHIPS = XS * YS
GROUP = CHIPS * CORES
JOINT_HEADS = HEADS + 2 * KV_HEADS
HALF_JOINT = JOINT_HEADS // CORES
GROUPS = KV_HEADS // CORES
UNITS = JOINT_HEADS // KV_HEADS
JOINT_AT = (0, 2, 4, 6, 9, 11, 13)
HEAD_AT = (4, 6, 0, 2, 13)
FAR_FIRST = (4, 3, 5, 2, 6, 1, 7, 0)
HALF_HEADS = HEADS // CORES
MESH = pl.DeviceIdType.MESH
F32, BF16 = jnp.float32, jnp.bfloat16


def position(within, places):
    at, ok = 0, False
    for r, p in enumerate(places):
        at = jnp.where(within == p, r, at)
        ok = jnp.logical_or(ok, within == p)
    return at, ok


def own_gain(gain, me, width):
    start = me * width
    tile, off = lax.div(start, LANES), lax.rem(start, LANES)
    line = lax.broadcasted_iota(jnp.int32, gain.shape, 0)
    lane = lax.broadcasted_iota(jnp.int32, (1, LANES), 1)
    first = jnp.sum(jnp.where(line == tile, gain, 0.0), axis=0, keepdims=True)
    second = jnp.sum(jnp.where(line == tile + 1, gain, 0.0), axis=0, keepdims=True)
    both = jnp.where(lane >= off, first, second)
    return pltpu.roll(jnp.broadcast_to(both, (ROWS, LANES)), lax.rem(LANES - off, LANES), 1)


def lanes_of(n):
    return pl.ds(pl.multiple_of(n * LANES, LANES), LANES)


def send(src, dst, send_sem, recv_sem, device):
    copy = pltpu.make_async_remote_copy(
        src_ref=src,
        dst_ref=dst,
        send_sem=send_sem,
        recv_sem=recv_sem,
        device_id={"seq": device},
        device_id_type=MESH,
    )
    copy.start()


def packed(value, level):
    lane = lax.broadcasted_iota(jnp.int32, (ROWS, LANES), 1)
    first = level.astype(BF16).astype(F32)
    second = (level - first).astype(BF16).astype(F32)
    third = level - first - second
    quarter = LANES // 4
    parts = jnp.where(
        lane < quarter, first,
        jnp.where(lane < 2 * quarter, second, jnp.where(lane < 3 * quarter, third, 0.0)),
    )
    return jnp.concatenate([value, parts], axis=0).astype(BF16)


def wait_bytes(ref, sem):
    pltpu.make_async_copy(ref, ref, sem).wait()


def cut_pieces(tiles, width, count):
    lane = lax.broadcasted_iota(jnp.int32, (ROWS, LANES), 1)
    pieces = []
    for j in range(count):
        t, off = divmod(width * j, LANES)
        piece = tiles[t] if off == 0 else pltpu.roll(tiles[t], LANES - off, 1)
        if off + width > LANES:
            rest = pltpu.roll(tiles[t + 1], LANES - off, 1)
            piece = jnp.where(lane < LANES - off, piece, rest)
        pieces.append(piece)
    return pieces


def join_pieces(pieces, width, tiles):
    lane = lax.broadcasted_iota(jnp.int32, (ROWS, LANES), 1)
    out = [None] * tiles

    def put(t, value):
        out[t] = value if out[t] is None else out[t] + value

    for j, piece in enumerate(pieces):
        t, off = divmod(width * j, LANES)
        moved = piece if off == 0 else pltpu.roll(piece, off, 1)
        if off + width > LANES:
            put(t, jnp.where(lane >= off, moved, 0.0))
            put(t + 1, jnp.where(lane < off, moved, 0.0))
        else:
            put(t, moved)
    return out


def kernel(
    ids_ref, len_ref, freq_ref, table_hbm, gain_ref, wqkv_hbm, bias_ref, keys_hbm, values_hbm,
    wout_hbm, mgain_ref, wgate_hbm, wup_hbm, wdown_hbm,
    att_ref, lay_ref,
    table, wqkv, keys, values, wout, wgate, wup, wdown,
    a1s, a1r, q1s, q1r, a2s, a2r, cosr, sinr,
    po, bx, bs, br, jflat,
    oo, ow, cx, cs, cr, levels, aflat, tmp, ds_, dx, mb, nflat,
    es, er, e2s, e2r, dummy,
    tsem, wsem, ssem, rsem, bxsem, jsem, cxsem,
):
    me = lax.axis_index("seq")
    x = lax.div(me, PLANE)
    j0 = lax.rem(me, PLANE)
    y = lax.div(j0, CORES)
    chip = lax.div(me, CORES)
    c = lax.rem(me, CORES)
    other = me + 1 - 2 * c
    width = lay_ref.shape[1]
    block = PLANE * width
    tiles = block // LANES
    vocab_rows = table.shape[1]
    group = HEADS // KV_HEADS

    x_peers = [(k, lax.rem(x + k, XS)) for k in FAR_FIRST[:-1]]
    y_part = [lax.rem(y + k, YS) * CORES for k in range(YS)]
    x_part = [lax.rem(x + k, XS) * PLANE for k in range(XS)]
    plane_peers = [
        (k, e, y_part[k] + lax.rem(c + e, CORES))
        for k in FAR_FIRST for e in range(CORES) if k or e
    ]
    chip_peers = sorted(
        [(i, j) for i in range(XS) for j in range(YS) if i or j],
        key=lambda p: -min(p[0], XS - p[0]) - min(p[1], YS - p[1]),
    )

    def to_all(tile, send_sem, recv_sem):
        for i, j in chip_peers:
            for e in range(CORES):
                send(tile, tile, send_sem, recv_sem, x_part[i] + y_part[j] + e)
        send(tile, tile, send_sem, recv_sem, other)

    barrier = pltpu.get_barrier_semaphore()
    for _, p in x_peers:
        pl.semaphore_signal(barrier, inc=1, device_id={"seq": p * PLANE + j0}, device_id_type=MESH)
    for _, _, p in plane_peers:
        pl.semaphore_signal(barrier, inc=1, device_id={"seq": x * PLANE + p}, device_id_type=MESH)
    order = [p for _, p in x_peers] + [x]
    loads = []
    for k, p in enumerate(order):
        at = pl.ds(pl.multiple_of(p * block, LANES), block)
        loads.append(pltpu.make_async_copy(table_hbm.at[:, at], table.at[k], tsem.at[k]))
        loads[-1].start()
    weights = [
        pltpu.make_async_copy(src, dst, wsem.at[k])
        for k, (src, dst) in enumerate(
            [(wqkv_hbm, wqkv), (keys_hbm, keys), (values_hbm, values), (wout_hbm, wout),
             (wgate_hbm, wgate), (wup_hbm, wup), (wdown_hbm, wdown)]
        )
    ]
    for w in weights:
        w.start()

    lane = lax.broadcasted_iota(jnp.int32, (ROWS, LANES), 1)
    row = lax.broadcasted_iota(jnp.int32, (ROWS, LANES), 0)
    low = lane < LANES // 2
    prompts = len_ref.shape[0]

    local = jnp.full((ROWS, vocab_rows), -1, jnp.int32)
    vrow = lax.broadcasted_iota(jnp.int32, (ROWS, vocab_rows), 0)
    vcol = lax.broadcasted_iota(jnp.int32, (ROWS, vocab_rows), 1)
    for r in range(ROWS):
        local = jnp.where(vrow == r, ids_ref[r % prompts, r // prompts] - me * vocab_rows, local)
    chosen = jnp.where(local == vcol, 1.0, 0.0).astype(BF16)
    square = jnp.zeros((ROWS, LANES), F32)
    for k in range(XS):
        loads[k].wait()
        found = jnp.dot(chosen, table[k], preferred_element_type=F32)
        a1s[k] = found.astype(BF16)
        for t in range(tiles):
            v = found[:, t * LANES : (t + 1) * LANES]
            square = square + v * v
        if k == 0:
            pl.semaphore_wait(barrier, XS + PLANE - 2)
        if k < XS - 1:
            d, p = x_peers[k]
            send(a1s.at[k], a1r.at[d - 1], ssem.at[0], rsem.at[0], p * PLANE + j0)
    q1s[...] = jnp.broadcast_to(
        jnp.sum(square, axis=-1, keepdims=True) / (XS * block), (ROWS, LANES)
    )
    for d, p in x_peers:
        send(q1s, q1r.at[d - 1], ssem.at[1], rsem.at[1], p * PLANE + j0)

    place = jnp.zeros((ROWS, LANES), jnp.int32)
    for r in range(ROWS):
        place = jnp.where(row == r, len_ref[r % prompts] + r // prompts, place)
    angle = place.astype(F32) * freq_ref[...]
    cosr[...] = jnp.cos(angle)
    sine = jnp.sin(angle)
    sinr[...] = jnp.where(lane < HEAD_DIM // 2, -sine, sine)

    wait_bytes(a1r, rsem.at[0])
    wait_bytes(q1r, rsem.at[1])
    total = a1s[XS - 1].astype(F32)
    for k in range(XS - 1):
        total = total + a1r[k].astype(F32)
    found = [total[:, t * LANES : (t + 1) * LANES] for t in range(tiles)]
    square = q1s[...] + jnp.sum(q1r[...], axis=0)
    for j, piece in enumerate(cut_pieces(found, width, PLANE)):
        a2s[j] = jnp.where(low, piece, square)
    for k, e, p in plane_peers:
        send(a2s.at[p], a2r.at[k * CORES + e - 1], ssem.at[2], rsem.at[2], x * PLANE + p)
    weights[0].wait()
    gain = own_gain(gain_ref[...].astype(F32), me, width)
    wait_bytes(a2r, rsem.at[2])
    stream = a2s[j0] + jnp.sum(a2r[...], axis=0)
    scale = lax.rsqrt(jnp.broadcast_to(stream[:, LANES - 1 :], (ROWS, LANES)) + NORM_EPS)
    normed = (stream * scale * gain).astype(BF16)[:, :width]

    half_group = lax.div(chip, CHIPS // GROUPS)
    within = lax.rem(chip, CHIPS // GROUPS)
    far_groups = [lax.rem(half_group + k, GROUPS) for k in (2, 1, 3, 0)]
    near_groups = [lax.rem(half_group + k, GROUPS) for k in (0, 1, 3, 2)]

    def project(side, g):
        starts = [
            (HALF_HEADS * side + group * g, group),
            (HEADS + GROUPS * side + g, 1),
            (HEADS + KV_HEADS + GROUPS * side + g, 1),
        ]
        out = []
        for at, n in starts:
            cols = pl.ds(pl.multiple_of(at * LANES, LANES), n * LANES)
            got = jnp.dot(normed, wqkv[:, cols], preferred_element_type=F32)
            out += [got[:, t * LANES : (t + 1) * LANES] for t in range(n)]
        return out

    for n, g in enumerate(far_groups):
        for r, v in enumerate(project(1 - c, g)):
            po[n, r] = v
        send(po.at[n], bx.at[n], ssem.at[4], bxsem.at[n], other)
    for n, g in enumerate(far_groups):
        mine = project(c, g)
        wait_bytes(bx.at[n], bxsem.at[n])
        for r in range(UNITS):
            bs[n, r] = mine[r] + bx[n, r]
        for r in range(UNITS):
            p = (CHIPS // GROUPS) * g + JOINT_AT[r]

            def go(n=n, r=r, p=p):
                slot = lax.rem(chip - p + CHIPS, CHIPS) - 1
                send(bs.at[n, r], br.at[slot], ssem.at[5], rsem.at[5], p * CORES + c)

            if n < GROUPS - 1:
                go()
            else:
                pl.when(within != JOINT_AT[r])(go)

    rb, b_on = position(within, JOINT_AT)
    nb = UNITS * (GROUPS * c + half_group) + rb

    @pl.when(b_on)
    def _():
        wait_bytes(br, rsem.at[5])
        at = jnp.where(
            rb < group, HALF_HEADS * c + group * half_group + rb,
            HEADS + GROUPS * c + half_group + jnp.where(rb > group, KV_HEADS, 0),
        )
        total = bs[GROUPS - 1, rb].astype(F32)
        for k in range(CHIPS - 1):
            total = total + br[k].astype(F32)
        total = total + bias_ref[pl.ds(at, 1), :]
        joint = total.astype(BF16).astype(F32)
        turned = joint * cosr[...] + pltpu.roll(joint, HEAD_DIM // 2, 1) * sinr[...]
        turn = jnp.where(rb <= group, 1.0, 0.0)
        jflat[:, lanes_of(nb)] = jnp.where(turn > 0.5, turned, joint).astype(BF16)
        tile = jflat.at[:, lanes_of(nb)]
        to_all(tile, ssem.at[6], jsem.at[GROUPS * c + half_group])

    weights[1].wait()
    weights[2].wait()
    span = keys.shape[1]
    lines = group * ROWS
    wide_row = lax.broadcasted_iota(jnp.int32, (lines, span), 0)
    even = lax.rem(wide_row, prompts) == 0
    where = me * span + lax.broadcasted_iota(jnp.int32, (lines, span), 1)
    valid = where < jnp.where(even, len_ref[0], len_ref[1])
    score_scale = 1.0 / math.sqrt(HEAD_DIM)
    nt = (((1,), (1,)), ((), ()))

    def attend(side, g, into):
        kv = GROUPS * side + g
        base = UNITS * kv
        at = lanes_of(kv)
        query = jnp.concatenate(
            [jflat[:, lanes_of(base + r)].astype(F32) for r in range(group)], axis=0
        ).astype(BF16)
        score = [
            lax.dot_general(query, keys[b, :, at], nt, preferred_element_type=F32)
            for b in range(prompts)
        ]
        score = jnp.where(valid, jnp.where(even, score[0], score[1]) * score_scale, MASKED)
        top = jnp.max(score, axis=-1, keepdims=True)
        weight = jnp.where(valid, jnp.exp(score - top), 0.0)
        total = jnp.sum(weight, axis=-1, keepdims=True)
        summed = jnp.dot(
            jnp.where(even, weight, 0.0).astype(BF16), values[0, :, at], preferred_element_type=F32
        ) + jnp.dot(
            jnp.where(even, 0.0, weight).astype(BF16), values[1, :, at], preferred_element_type=F32
        )
        top = jnp.broadcast_to(top, (lines, LANES))
        total = jnp.broadcast_to(total, (lines, LANES))
        for r in range(group):
            into[r, 0] = summed[r * ROWS : (r + 1) * ROWS]
            into[r, 1] = top[r * ROWS : (r + 1) * ROWS]
            into[r, 2] = total[r * ROWS : (r + 1) * ROWS]

    def joint_group(kv):
        return jflat.at[:, pl.ds(pl.multiple_of(kv * UNITS * LANES, LANES), UNITS * LANES)]

    def merge(n, g):
        wait_bytes(cx.at[n], cxsem.at[n])
        for r in range(group):
            top_a, top_b = ow[n, r, 1], cx[n, r, 1]
            top = jnp.maximum(top_a, top_b)
            scale_a, scale_b = jnp.exp(top_a - top), jnp.exp(top_b - top)
            summed = ow[n, r, 0] * scale_a + cx[n, r, 0] * scale_b
            total = ow[n, r, 2] * scale_a + cx[n, r, 2] * scale_b
            some = total > 0.0
            total = jnp.where(some, total, 1.0)
            level = jnp.where(some, top + jnp.log(total), MASKED)
            cs[n, r] = packed(jnp.where(some, summed / total, 0.0), level)
        across = lax.rem(g + GROUPS // 2, GROUPS)
        for r in range(group):
            p = (CHIPS // GROUPS) * across + HEAD_AT[r]

            def go(r=r, p=p):
                slot = lax.rem(chip - p + CHIPS, CHIPS) - 1
                send(cs.at[n, r], cr.at[slot], ssem.at[8], rsem.at[8], p * CORES + c)

            if n < GROUPS - 1:
                go()
            else:
                pl.when(within != HEAD_AT[r])(go)

    for n, g in enumerate(near_groups):
        kv = GROUPS * (1 - c) + g
        wait_bytes(joint_group(kv), jsem.at[kv])
        attend(1 - c, g, oo.at[n])
        send(oo.at[n], cx.at[n], ssem.at[7], cxsem.at[n], other)
        kv = GROUPS * c + g
        if n == 0:
            @pl.when(b_on)
            def _(kv=kv):
                part = pl.ds(pl.multiple_of(kv * UNITS * LANES, LANES), (UNITS - 1) * LANES)
                wait_bytes(jflat.at[:, part], jsem.at[kv])

            @pl.when(jnp.logical_not(b_on))
            def _(kv=kv):
                wait_bytes(joint_group(kv), jsem.at[kv])
        else:
            wait_bytes(joint_group(kv), jsem.at[kv])
        attend(c, g, ow.at[n])
        if n:
            merge(n - 1, near_groups[n - 1])
    merge(GROUPS - 1, near_groups[-1])

    rc, c_on = position(within, HEAD_AT)
    gc = lax.rem(half_group + GROUPS // 2, GROUPS)
    hc = HALF_HEADS * c + group * gc + rc

    @pl.when(c_on)
    def _():
        base = UNITS * (GROUPS * c + gc)
        query = jflat[:, lanes_of(base + rc)]
        new_key = jflat[:, lanes_of(base + group)]
        new_value = jflat[:, lanes_of(base + group + 1)]
        small_r = lax.broadcasted_iota(jnp.int32, (ROWS, ROWS), 0)
        small_c = lax.broadcasted_iota(jnp.int32, (ROWS, ROWS), 1)
        seen = jnp.logical_and(
            small_c <= small_r, lax.rem(small_c, prompts) == lax.rem(small_r, prompts)
        )
        score = lax.dot_general(query, new_key, nt, preferred_element_type=F32) * score_scale
        score = jnp.where(seen, score, MASKED)
        top = jnp.max(score, axis=-1, keepdims=True)
        weight = jnp.where(seen, jnp.exp(score - top), 0.0)
        total = jnp.sum(weight, axis=-1, keepdims=True)
        new_sum = jnp.dot(weight.astype(BF16), new_value, preferred_element_type=F32)
        best = top + jnp.log(total)
        levels[CHIPS] = jnp.broadcast_to(best, (ROWS, LANES))
        best = levels[CHIPS]
        wait_bytes(cr, rsem.at[8])

        def partial(s):
            return cs[GROUPS - 1, rc] if s == CHIPS - 1 else cr[s]

        for s in range(CHIPS):
            level = partial(s)[ROWS:].astype(F32)
            level = level + pltpu.roll(level, LANES // 2, 1)
            level = level + pltpu.roll(level, LANES // 4, 1)
            levels[s] = level
            best = jnp.maximum(best, level)
        den = jnp.exp(levels[CHIPS] - best)
        acc = new_sum / total * den
        for s in range(CHIPS):
            scale = jnp.exp(levels[s] - best)
            acc = acc + partial(s)[:ROWS].astype(F32) * scale
            den = den + scale
        aflat[:, lanes_of(hc)] = (acc / den).astype(BF16)
        to_all(aflat.at[:, lanes_of(hc)], ssem.at[9], rsem.at[9])
        wait_bytes(aflat.at[:, : (HEADS - 1) * LANES], rsem.at[9])

    @pl.when(jnp.logical_not(c_on))
    def _():
        wait_bytes(aflat, rsem.at[9])

    weights[3].wait()
    attended = aflat[...]
    tmp[...] = jnp.zeros((ROWS, LANES), F32)
    tmp[:, :width] = lax.dot_general(attended, wout[...], nt, preferred_element_type=F32)
    mid = jnp.where(lane < width, tmp[...] + stream, 0.0)
    mine = jnp.where(lax.rem(row * 0 + c, CORES) == 0, mid, pltpu.roll(mid, width, 1))
    ds_[...] = mine
    send(ds_, dx, ssem.at[10], rsem.at[10], other)
    wait_bytes(dx, rsem.at[10])
    mb[chip] = (mine + dx[...]).astype(BF16)
    for i, j in chip_peers:
        send(mb.at[chip], mb.at[chip], ssem.at[11], rsem.at[11], x_part[i] + y_part[j] + c)

    att_ref[...] = attended
    weights[4].wait()
    weights[5].wait()
    weights[6].wait()
    wait_bytes(mb.at[pl.ds(0, CHIPS - 1)], rsem.at[11])
    mids = join_pieces([mb[p].astype(F32) for p in range(CHIPS)], CORES * width, XS * tiles)
    square = jnp.zeros((ROWS, LANES), F32)
    for v in mids:
        square = square + v * v
    scale = lax.rsqrt(jnp.sum(square, axis=-1, keepdims=True) / (XS * block) + NORM_EPS)
    gain = mgain_ref[...].astype(F32)
    for g, v in enumerate(mids):
        nflat[:, g * LANES : (g + 1) * LANES] = (v * scale * gain[g : g + 1, :]).astype(BF16)
    normed_mid = nflat[...]
    gate = jnp.dot(normed_mid, wgate[...], preferred_element_type=F32)
    upper = jnp.dot(normed_mid, wup[...], preferred_element_type=F32)
    hidden = (gate / (1.0 + jnp.exp(-gate)) * upper).astype(BF16)
    for k, p in enumerate(order):
        at = pl.ds(pl.multiple_of(p * block, LANES), block)
        es[k] = jnp.dot(hidden, wdown[:, at], preferred_element_type=F32).astype(BF16)
        if k < XS - 1:
            d = x_peers[k][0]
            send(es.at[k], er.at[d - 1], ssem.at[12], rsem.at[12], p * PLANE + j0)
    wait_bytes(er, rsem.at[12])
    total = es[XS - 1].astype(F32)
    for k in range(XS - 1):
        total = total + er[k].astype(F32)
    found = [total[:, t * LANES : (t + 1) * LANES] for t in range(tiles)]
    for j, piece in enumerate(cut_pieces(found, width, PLANE)):
        e2s[j] = piece
    for k, e, p in plane_peers:
        send(e2s.at[p], e2r.at[k * CORES + e - 1], ssem.at[13], rsem.at[13], x * PLANE + p)
    wait_bytes(e2r, rsem.at[13])
    final = mid + e2s[j0] + jnp.sum(e2r[...], axis=0)
    lay_ref[...] = final[:, :width].astype(BF16)

    for sem, ref in (
        (0, a1r), (1, q1r), (2, a2r), (4, bx), (7, cx), (10, dx), (12, er), (13, e2r),
    ):
        wait_bytes(ref, ssem.at[sem])
    wait_bytes(mb.at[pl.ds(0, CHIPS - 1)], ssem.at[11])

    @pl.when(b_on)
    def _():
        wait_bytes(br.at[pl.ds(0, HALF_JOINT - 1)], ssem.at[5])
        wait_bytes(dummy, ssem.at[6])

    @pl.when(jnp.logical_not(b_on))
    def _():
        wait_bytes(br.at[pl.ds(0, HALF_JOINT)], ssem.at[5])

    @pl.when(c_on)
    def _():
        wait_bytes(cr.at[pl.ds(0, HALF_HEADS - 1)], ssem.at[8])
        wait_bytes(dummy, ssem.at[9])

    @pl.when(jnp.logical_not(c_on))
    def _():
        wait_bytes(cr.at[pl.ds(0, HALF_HEADS)], ssem.at[8])


def body(
    token_ids, lengths, embed_table, attn_gain, w_qkv, qkv_bias, cache_keys, cache_values, w_out,
    mlp_gain, w_gate, w_up, w_down,
):
    steps, prompts = token_ids.shape
    vocab_rows, model = embed_table.shape
    width = w_out.shape[1]
    block = PLANE * width
    per_group = HEADS // KV_HEADS
    half = HEAD_DIM // 2
    frequency = np.float32(ROPE_BASE) ** (
        np.float32(-2.0) * np.arange(half, dtype=np.float32) / np.float32(HEAD_DIM)
    )
    frequency = jnp.asarray(np.tile(np.concatenate([frequency, frequency]), (ROWS, 1)), F32)
    vmem = pl.BlockSpec(memory_space=pltpu.VMEM)
    smem = pl.BlockSpec(memory_space=pltpu.SMEM)
    hbm = pl.BlockSpec(memory_space=pl.ANY)
    w_out_t = w_out.T

    def like(a):
        return pltpu.VMEM(a.shape, a.dtype)

    def tile(*lead, dtype=F32):
        return pltpu.VMEM((*lead, ROWS, LANES), dtype)

    def wide(*lead, dtype):
        return pltpu.VMEM((*lead, ROWS, block), dtype)

    attended, layer_out = pl.pallas_call(
        kernel,
        out_shape=(
            jax.ShapeDtypeStruct((ROWS, HEADS * HEAD_DIM), BF16),
            jax.ShapeDtypeStruct((ROWS, width), BF16),
        ),
        in_specs=[smem, smem, vmem, hbm, vmem, hbm, vmem, hbm, hbm, hbm, vmem, hbm, hbm, hbm],
        out_specs=(vmem, vmem),
        scratch_shapes=[
            pltpu.VMEM((XS, vocab_rows, block), BF16),
            like(w_qkv), like(cache_keys), like(cache_values), like(w_out_t),
            like(w_gate), like(w_up), like(w_down),
            wide(XS, dtype=BF16), wide(XS - 1, dtype=BF16), tile(), tile(XS - 1),
            tile(PLANE), tile(PLANE - 1), tile(), tile(),
            tile(GROUPS, UNITS), tile(GROUPS, UNITS), tile(GROUPS, UNITS),
            tile(CHIPS - 1),
            pltpu.VMEM((ROWS, JOINT_HEADS * LANES), BF16),
            tile(GROUPS, per_group, 3), tile(GROUPS, per_group, 3), tile(GROUPS, per_group, 3),
            pltpu.VMEM((GROUPS, per_group, 2 * ROWS, LANES), BF16),
            pltpu.VMEM((CHIPS - 1, 2 * ROWS, LANES), BF16), tile(CHIPS + 1),
            pltpu.VMEM((ROWS, HEADS * LANES), BF16),
            tile(), tile(), tile(), tile(CHIPS, dtype=BF16),
            pltpu.VMEM((ROWS, model), BF16),
            wide(XS, dtype=BF16), wide(XS - 1, dtype=BF16), tile(PLANE), tile(PLANE - 1),
            tile(GROUP - 1, dtype=BF16),
            pltpu.SemaphoreType.DMA((XS,)),
            pltpu.SemaphoreType.DMA((7,)),
            pltpu.SemaphoreType.DMA((14,)),
            pltpu.SemaphoreType.DMA((14,)),
            pltpu.SemaphoreType.DMA((GROUPS,)),
            pltpu.SemaphoreType.DMA((KV_HEADS,)),
            pltpu.SemaphoreType.DMA((GROUPS,)),
        ],
        compiler_params=pltpu.CompilerParams(
            collective_id=0, has_side_effects=True, vmem_limit_bytes=60 * 2**20
        ),
        name="layer",
    )(
        token_ids.T, lengths, frequency, embed_table, attn_gain.reshape(-1, LANES), w_qkv,
        qkv_bias.reshape(-1, LANES), cache_keys, cache_values, w_out_t,
        mlp_gain.reshape(-1, LANES), w_gate, w_up, w_down,
    )
    return (
        attended.reshape(steps, prompts, -1),
        layer_out.reshape(steps, prompts, width),
    )


def solution(mesh):
    return jax.shard_map(
        body,
        mesh=mesh,
        in_specs=(
            P(None, "parts"), P("parts"), P("seq", None), P(), P("seq", None), P(),
            P("parts", "seq", None), P("parts", "seq", None), P(None, "seq"), P(),
            P(None, "seq"), P(None, "seq"), P("seq", None),
        ),
        out_specs=(P(None, "parts", None), P(None, "parts", "seq")),
        check_vma=False,
    )
```

```python
import functools
import math

import jax
import jax.numpy as jnp
import numpy as np
from jax import lax
from jax.experimental import pallas as pl
from jax.experimental.pallas import tpu as pltpu
from jax.sharding import PartitionSpec as P

HEADS = 40
KV_HEADS = 8
HEAD_DIM = 128
NORM_EPS = 1e-06
ROPE_BASE = 1000000.0
MASKED = -1e30

ROWS = 8
LANES = 128
XS, YS, CORES = 8, 8, 2
PLANE = YS * CORES
CHIPS = XS * YS
GROUP = CHIPS * CORES
JOINT_HEADS = HEADS + 2 * KV_HEADS
HALF_JOINT = JOINT_HEADS // CORES
GROUPS = KV_HEADS // CORES
UNITS = JOINT_HEADS // KV_HEADS
JOINT_AT = (0, 2, 4, 6, 9, 11, 13)
HEAD_AT = (4, 6, 0, 2, 13)
FAR_FIRST = (4, 3, 5, 2, 6, 1, 7, 0)
HALF_HEADS = HEADS // CORES
MESH = pl.DeviceIdType.MESH
F32, BF16 = jnp.float32, jnp.bfloat16


def position(within, places):
    at, ok = 0, False
    for r, p in enumerate(places):
        at = jnp.where(within == p, r, at)
        ok = jnp.logical_or(ok, within == p)
    return at, ok


def own_gain(gain, me, width):
    start = me * width
    tile, off = lax.div(start, LANES), lax.rem(start, LANES)
    line = lax.broadcasted_iota(jnp.int32, gain.shape, 0)
    lane = lax.broadcasted_iota(jnp.int32, (1, LANES), 1)
    first = jnp.sum(jnp.where(line == tile, gain, 0.0), axis=0, keepdims=True)
    second = jnp.sum(jnp.where(line == tile + 1, gain, 0.0), axis=0, keepdims=True)
    both = jnp.where(lane >= off, first, second)
    return pltpu.roll(jnp.broadcast_to(both, (ROWS, LANES)), lax.rem(LANES - off, LANES), 1)


def lanes_of(n):
    return pl.ds(pl.multiple_of(n * LANES, LANES), LANES)


def send(src, dst, send_sem, recv_sem, device):
    copy = pltpu.make_async_remote_copy(
        src_ref=src,
        dst_ref=dst,
        send_sem=send_sem,
        recv_sem=recv_sem,
        device_id={"seq": device},
        device_id_type=MESH,
    )
    copy.start()


def packed(value, level):
    lane = lax.broadcasted_iota(jnp.int32, (ROWS, LANES), 1)
    first = level.astype(BF16).astype(F32)
    second = (level - first).astype(BF16).astype(F32)
    third = level - first - second
    quarter = LANES // 4
    parts = jnp.where(
        lane < quarter, first,
        jnp.where(lane < 2 * quarter, second, jnp.where(lane < 3 * quarter, third, 0.0)),
    )
    return jnp.concatenate([value, parts], axis=0).astype(BF16)


def wait_bytes(ref, sem):
    pltpu.make_async_copy(ref, ref, sem).wait()


def cut_pieces(tiles, width, count):
    lane = lax.broadcasted_iota(jnp.int32, (ROWS, LANES), 1)
    pieces = []
    for j in range(count):
        t, off = divmod(width * j, LANES)
        piece = tiles[t] if off == 0 else pltpu.roll(tiles[t], LANES - off, 1)
        if off + width > LANES:
            rest = pltpu.roll(tiles[t + 1], LANES - off, 1)
            piece = jnp.where(lane < LANES - off, piece, rest)
        pieces.append(piece)
    return pieces


def join_pieces(pieces, width, tiles):
    lane = lax.broadcasted_iota(jnp.int32, (ROWS, LANES), 1)
    out = [None] * tiles

    def put(t, value):
        out[t] = value if out[t] is None else out[t] + value

    for j, piece in enumerate(pieces):
        t, off = divmod(width * j, LANES)
        moved = piece if off == 0 else pltpu.roll(piece, off, 1)
        if off + width > LANES:
            put(t, jnp.where(lane >= off, moved, 0.0))
            put(t + 1, jnp.where(lane < off, moved, 0.0))
        else:
            put(t, moved)
    return out


def kernel(
    ids_ref, len_ref, freq_ref, table_hbm, gain_ref, wqkv_hbm, bias_ref, keys_hbm, values_hbm,
    wout_hbm, mgain_ref, wgate_hbm, wup_hbm, wdown_hbm,
    att_ref, lay_ref,
    table, wqkv, keys, values, wout, wgu, wdown,
    a1s, a1r, q1s, q1r, a2s, a2r, cosr, sinr,
    bs, br, jflat,
    cs, cr, levels, aflat, tmp, mb, nflat,
    es, er, e2s, e2r, dummy,
    tsem, wsem, ssem, rsem, jsem, osem, psem,
):
    me = lax.axis_index("seq")
    x = lax.div(me, PLANE)
    j0 = lax.rem(me, PLANE)
    y = lax.div(j0, CORES)
    chip = lax.div(me, CORES)
    c = lax.rem(me, CORES)
    other = me + 1 - 2 * c
    width = lay_ref.shape[1]
    block = PLANE * width
    tiles = block // LANES
    vocab_rows = table.shape[1]
    group = HEADS // KV_HEADS

    x_peers = [(k, lax.rem(x + k, XS)) for k in FAR_FIRST[:-1]]
    y_part = [lax.rem(y + k, YS) * CORES for k in range(YS)]
    x_part = [lax.rem(x + k, XS) * PLANE for k in range(XS)]
    plane_peers = [
        (k, e, y_part[k] + lax.rem(c + e, CORES))
        for k in FAR_FIRST for e in range(CORES) if k or e
    ]
    chip_peers = sorted(
        [(i, j) for i in range(XS) for j in range(YS) if i or j],
        key=lambda p: -min(p[0], XS - p[0]) - min(p[1], YS - p[1]),
    )

    def to_all(tile, send_sem, recv_sem):
        for i, j in chip_peers:
            for e in range(CORES):
                send(tile, tile, send_sem, recv_sem, x_part[i] + y_part[j] + e)
        send(tile, tile, send_sem, recv_sem, other)

    def to_core(tile, send_sem, recv_sem):
        for i, j in chip_peers:
            send(tile, tile, send_sem, recv_sem, x_part[i] + y_part[j] + c)

    barrier = pltpu.get_barrier_semaphore()
    for _, p in x_peers:
        pl.semaphore_signal(barrier, inc=1, device_id={"seq": p * PLANE + j0}, device_id_type=MESH)
    order = [p for _, p in x_peers] + [x]
    blocks = [pl.ds(pl.multiple_of(p * block, LANES), block) for p in order]
    loads = []
    for k, at in enumerate(blocks):
        loads.append(pltpu.make_async_copy(table_hbm.at[:, at], table.at[k], tsem.at[k]))
        loads[-1].start()
    for _, _, p in plane_peers:
        pl.semaphore_signal(barrier, inc=1, device_id={"seq": x * PLANE + p}, device_id_type=MESH)

    def parts(side):
        def cols(start, n):
            return pl.ds(pl.multiple_of(start * LANES, LANES), n * LANES)

        out = []
        for at, n, to in (
            (HALF_HEADS * side, HALF_HEADS, 0),
            (HEADS + GROUPS * side, GROUPS, HALF_HEADS),
            (HEADS + KV_HEADS + GROUPS * side, GROUPS, HALF_HEADS + GROUPS),
        ):
            out.append((wqkv_hbm.at[:, cols(at, n)], wqkv.at[c, :, cols(to, n)]))
        mine = cols(GROUPS * side, GROUPS)
        out.append((keys_hbm.at[:, :, mine], keys.at[c]))
        out.append((values_hbm.at[:, :, mine], values.at[c]))
        out.append((wout_hbm, wout.at[c]))
        return out

    weights = [
        pltpu.make_async_copy(src, dst, wsem.at[k])
        for k, (src, dst) in enumerate(
            parts(c) + [(wgate_hbm, wgu.at[:, :LANES]), (wup_hbm, wgu.at[:, LANES:])]
            + [(wdown_hbm.at[:, at], wdown.at[k]) for k, at in enumerate(blocks)]
        )
    ]
    for w in weights:
        w.start()
    swaps = [
        pltpu.make_async_remote_copy(
            src_ref=src, dst_ref=dst, send_sem=osem.at[k], recv_sem=psem.at[k],
            device_id={"seq": other}, device_id_type=MESH,
        )
        for k, (src, dst) in enumerate(parts(1 - c))
    ]

    lane = lax.broadcasted_iota(jnp.int32, (ROWS, LANES), 1)
    row = lax.broadcasted_iota(jnp.int32, (ROWS, LANES), 0)
    low = lane < LANES // 2
    prompts = len_ref.shape[0]

    local = jnp.full((ROWS, vocab_rows), -1, jnp.int32)
    vrow = lax.broadcasted_iota(jnp.int32, (ROWS, vocab_rows), 0)
    vcol = lax.broadcasted_iota(jnp.int32, (ROWS, vocab_rows), 1)
    for r in range(ROWS):
        local = jnp.where(vrow == r, ids_ref[r % prompts, r // prompts] - me * vocab_rows, local)
    chosen = jnp.where(local == vcol, 1.0, 0.0).astype(BF16)
    square = jnp.zeros((ROWS, LANES), F32)
    for k in range(XS):
        loads[k].wait()
        found = jnp.dot(chosen, table[k], preferred_element_type=F32)
        a1s[k] = found.astype(BF16)
        for t in range(tiles):
            v = found[:, t * LANES : (t + 1) * LANES]
            square = square + v * v
        if k == 0:
            pl.semaphore_wait(barrier, XS + PLANE - 2)
        if k < XS - 1:
            d, p = x_peers[k]
            send(a1s.at[k], a1r.at[d - 1], ssem.at[0], rsem.at[0], p * PLANE + j0)
    q1s[...] = jnp.broadcast_to(
        jnp.sum(square, axis=-1, keepdims=True) / (XS * block), (ROWS, LANES)
    )
    for d, p in x_peers:
        send(q1s, q1r.at[d - 1], ssem.at[1], rsem.at[1], p * PLANE + j0)
    for w in swaps:
        w.start()

    place = jnp.zeros((ROWS, LANES), jnp.int32)
    for r in range(ROWS):
        place = jnp.where(row == r, len_ref[r % prompts] + r // prompts, place)
    angle = place.astype(F32) * freq_ref[...]
    cosr[...] = jnp.cos(angle)
    sine = jnp.sin(angle)
    sinr[...] = jnp.where(lane < HEAD_DIM // 2, -sine, sine)

    wait_bytes(a1r, rsem.at[0])
    wait_bytes(q1r, rsem.at[1])
    total = a1s[XS - 1].astype(F32)
    for k in range(XS - 1):
        total = total + a1r[k].astype(F32)
    found = [total[:, t * LANES : (t + 1) * LANES] for t in range(tiles)]
    square = q1s[...] + jnp.sum(q1r[...], axis=0)
    pair = CORES * width
    for j, piece in enumerate(cut_pieces(found, pair, YS)):
        a2s[j] = jnp.where(lane < pair, piece, square)
    for k, e, p in plane_peers:
        to = lax.div(p, CORES)
        send(a2s.at[to], a2r.at[k * CORES + e - 1], ssem.at[2], rsem.at[2], x * PLANE + p)
    gain = own_gain(gain_ref[...].astype(F32), chip, pair)
    for k in range(3):
        weights[k].wait()
        swaps[k].wait_recv()
    wait_bytes(a2r, rsem.at[2])
    stream = a2s[y] + jnp.sum(a2r[...], axis=0)
    scale = lax.rsqrt(jnp.broadcast_to(stream[:, LANES - 1 :], (ROWS, LANES)) + NORM_EPS)
    normed = stream * scale * gain
    normed = [
        v[:, :width].astype(BF16) for v in (normed, pltpu.roll(normed, LANES - width, 1))
    ]

    half_group = lax.div(chip, CHIPS // GROUPS)
    within = lax.rem(chip, CHIPS // GROUPS)
    far_groups = [lax.rem(half_group + k, GROUPS) for k in (2, 1, 3, 0)]
    near_groups = [lax.rem(half_group + k, GROUPS) for k in (0, 1, 3, 2)]

    def project(at, n):
        cols = pl.ds(pl.multiple_of(at * LANES, LANES), n * LANES)
        got = sum(
            jnp.dot(normed[e], wqkv[e, :, cols], preferred_element_type=F32) for e in range(CORES)
        )
        return [got[:, t * LANES : (t + 1) * LANES] for t in range(n)]

    for n, g in enumerate(far_groups):
        mine = (
            project(group * g, group) + project(HALF_HEADS + g, 1)
            + project(HALF_HEADS + GROUPS + g, 1)
        )
        for r in range(UNITS):
            bs[n, r] = mine[r]
        for r in range(UNITS):
            p = (CHIPS // GROUPS) * g + JOINT_AT[r]

            def go(n=n, r=r, p=p):
                slot = lax.rem(chip - p + CHIPS, CHIPS) - 1
                send(bs.at[n, r], br.at[slot], ssem.at[5], rsem.at[5], p * CORES + c)

            if n < GROUPS - 1:
                go()
            else:
                pl.when(within != JOINT_AT[r])(go)

    rb, b_on = position(within, JOINT_AT)
    nb = UNITS * half_group + rb

    @pl.when(b_on)
    def _():
        wait_bytes(br, rsem.at[5])
        at = jnp.where(
            rb < group, HALF_HEADS * c + group * half_group + rb,
            HEADS + GROUPS * c + half_group + jnp.where(rb > group, KV_HEADS, 0),
        )
        total = bs[GROUPS - 1, rb].astype(F32)
        for k in range(CHIPS - 1):
            total = total + br[k].astype(F32)
        total = total + bias_ref[pl.ds(at, 1), :]
        joint = total.astype(BF16).astype(F32)
        turned = joint * cosr[...] + pltpu.roll(joint, HEAD_DIM // 2, 1) * sinr[...]
        turn = jnp.where(rb <= group, 1.0, 0.0)
        jflat[:, lanes_of(nb)] = jnp.where(turn > 0.5, turned, joint).astype(BF16)
        tile = jflat.at[:, lanes_of(nb)]
        to_core(tile, ssem.at[6], jsem.at[half_group])

    for k in range(3, 5):
        weights[k].wait()
        swaps[k].wait_recv()
    span = keys.shape[2]
    lines = group * ROWS
    wide_row = lax.broadcasted_iota(jnp.int32, (lines, CORES * span), 0)
    even = lax.rem(wide_row, prompts) == 0
    where = chip * (CORES * span) + lax.broadcasted_iota(jnp.int32, (lines, CORES * span), 1)
    valid = where < jnp.where(even, len_ref[0], len_ref[1])
    score_scale = 1.0 / math.sqrt(HEAD_DIM)
    nt = (((1,), (1,)), ((), ()))

    def joint_group(g, n=UNITS):
        return jflat.at[:, pl.ds(pl.multiple_of(g * UNITS * LANES, LANES), n * LANES)]

    for n, g in enumerate(near_groups):
        if n == 0:
            @pl.when(b_on)
            def _(g=g):
                wait_bytes(joint_group(g, UNITS - 1), jsem.at[g])

            @pl.when(jnp.logical_not(b_on))
            def _(g=g):
                wait_bytes(joint_group(g), jsem.at[g])
        else:
            wait_bytes(joint_group(g), jsem.at[g])
        at = lanes_of(g)
        query = jnp.concatenate(
            [jflat[:, lanes_of(UNITS * g + r)].astype(F32) for r in range(group)], axis=0
        ).astype(BF16)
        score = [
            jnp.concatenate(
                [
                    lax.dot_general(query, keys[e, b, :, at], nt, preferred_element_type=F32)
                    for e in range(CORES)
                ],
                axis=1,
            )
            for b in range(prompts)
        ]
        score = jnp.where(valid, jnp.where(even, score[0], score[1]) * score_scale, MASKED)
        top = jnp.max(score, axis=-1, keepdims=True)
        weight = jnp.where(valid, jnp.exp(score - top), 0.0)
        total = jnp.sum(weight, axis=-1, keepdims=True)
        split = [
            jnp.where(even, weight, 0.0).astype(BF16), jnp.where(even, 0.0, weight).astype(BF16)
        ]
        summed = sum(
            jnp.dot(
                split[b][:, e * span : (e + 1) * span], values[e, b, :, at],
                preferred_element_type=F32,
            )
            for b in range(prompts)
            for e in range(CORES)
        )
        some = total > 0.0
        total = jnp.where(some, total, 1.0)
        level = jnp.broadcast_to(
            jnp.where(some, top + jnp.log(total), MASKED), (lines, LANES)
        )
        summed = summed / total
        for r in range(group):
            own = slice(r * ROWS, (r + 1) * ROWS)
            cs[n, r] = packed(summed[own], level[own])
        across = lax.rem(g + GROUPS // 2, GROUPS)
        for r in range(group):
            p = (CHIPS // GROUPS) * across + HEAD_AT[r]

            def go(n=n, r=r, p=p):
                slot = lax.rem(chip - p + CHIPS, CHIPS) - 1
                send(cs.at[n, r], cr.at[slot], ssem.at[8], rsem.at[8], p * CORES + c)

            if n < GROUPS - 1:
                go()
            else:
                pl.when(within != HEAD_AT[r])(go)

    rc, c_on = position(within, HEAD_AT)
    gc = lax.rem(half_group + GROUPS // 2, GROUPS)
    hc = HALF_HEADS * c + group * gc + rc

    @pl.when(c_on)
    def _():
        base = UNITS * gc
        query = jflat[:, lanes_of(base + rc)]
        new_key = jflat[:, lanes_of(base + group)]
        new_value = jflat[:, lanes_of(base + group + 1)]
        small_r = lax.broadcasted_iota(jnp.int32, (ROWS, ROWS), 0)
        small_c = lax.broadcasted_iota(jnp.int32, (ROWS, ROWS), 1)
        seen = jnp.logical_and(
            small_c <= small_r, lax.rem(small_c, prompts) == lax.rem(small_r, prompts)
        )
        score = lax.dot_general(query, new_key, nt, preferred_element_type=F32) * score_scale
        score = jnp.where(seen, score, MASKED)
        top = jnp.max(score, axis=-1, keepdims=True)
        weight = jnp.where(seen, jnp.exp(score - top), 0.0)
        total = jnp.sum(weight, axis=-1, keepdims=True)
        new_sum = jnp.dot(weight.astype(BF16), new_value, preferred_element_type=F32)
        best = top + jnp.log(total)
        levels[CHIPS] = jnp.broadcast_to(best, (ROWS, LANES))
        best = levels[CHIPS]
        wait_bytes(cr, rsem.at[8])

        def partial(s):
            return cs[GROUPS - 1, rc] if s == CHIPS - 1 else cr[s]

        for s in range(CHIPS):
            level = partial(s)[ROWS:].astype(F32)
            level = level + pltpu.roll(level, LANES // 2, 1)
            level = level + pltpu.roll(level, LANES // 4, 1)
            levels[s] = level
            best = jnp.maximum(best, level)
        den = jnp.exp(levels[CHIPS] - best)
        acc = new_sum / total * den
        for s in range(CHIPS):
            scale = jnp.exp(levels[s] - best)
            acc = acc + partial(s)[:ROWS].astype(F32) * scale
            den = den + scale
        aflat[:, lanes_of(hc)] = (acc / den).astype(BF16)
        to_all(aflat.at[:, lanes_of(hc)], ssem.at[9], rsem.at[9])
        wait_bytes(aflat.at[:, : (HEADS - 1) * LANES], rsem.at[9])

    @pl.when(jnp.logical_not(c_on))
    def _():
        wait_bytes(aflat, rsem.at[9])

    weights[5].wait()
    swaps[5].wait_recv()
    attended = aflat[...]
    tmp[...] = jnp.zeros((ROWS, LANES), F32)
    for e in range(CORES):
        tmp[:, e * width : (e + 1) * width] = lax.dot_general(
            attended, wout[e], nt, preferred_element_type=F32
        )
    mid = jnp.where(lane < pair, tmp[...] + stream, 0.0)
    mb[chip] = mid.astype(BF16)
    to_core(mb.at[chip], ssem.at[11], rsem.at[11])

    att_ref[...] = attended
    for w in weights[6:]:
        w.wait()
    wait_bytes(mb.at[pl.ds(0, CHIPS - 1)], rsem.at[11])
    mids = join_pieces([mb[p].astype(F32) for p in range(CHIPS)], pair, XS * tiles)
    square = jnp.zeros((ROWS, LANES), F32)
    for v in mids:
        square = square + v * v
    scale = lax.rsqrt(jnp.sum(square, axis=-1, keepdims=True) / (XS * block) + NORM_EPS)
    gain = mgain_ref[...].astype(F32)
    for g, v in enumerate(mids):
        nflat[:, g * LANES : (g + 1) * LANES] = (v * scale * gain[g : g + 1, :]).astype(BF16)
    normed_mid = nflat[...]
    both = jnp.dot(normed_mid, wgu[...], preferred_element_type=F32)
    gate, upper = both[:, :LANES], both[:, LANES:]
    hidden = (gate / (1.0 + jnp.exp(-gate)) * upper).astype(BF16)
    for k, p in enumerate(order):
        es[k] = jnp.dot(hidden, wdown[k], preferred_element_type=F32).astype(BF16)
        if k < XS - 1:
            d = x_peers[k][0]
            send(es.at[k], er.at[d - 1], ssem.at[12], rsem.at[12], p * PLANE + j0)
    wait_bytes(er, rsem.at[12])
    total = es[XS - 1].astype(F32)
    for k in range(XS - 1):
        total = total + er[k].astype(F32)
    found = [total[:, t * LANES : (t + 1) * LANES] for t in range(tiles)]
    for j, piece in enumerate(cut_pieces(found, width, PLANE)):
        e2s[j] = piece.astype(BF16)
    for k, e, p in plane_peers:
        send(e2s.at[p], e2r.at[k * CORES + e - 1], ssem.at[13], rsem.at[13], x * PLANE + p)
    wait_bytes(e2r, rsem.at[13])
    final = e2s[j0].astype(F32)
    for k in range(PLANE - 1):
        final = final + e2r[k].astype(F32)
    final = final + jnp.where(row * 0 + c == 0, mid, pltpu.roll(mid, LANES - width, 1))
    lay_ref[...] = final[:, :width].astype(BF16)

    for sem, ref in (
        (0, a1r), (1, q1r), (2, a2r), (12, er), (13, e2r),
    ):
        wait_bytes(ref, ssem.at[sem])
    wait_bytes(mb.at[pl.ds(0, CHIPS - 1)], ssem.at[11])
    for w in swaps:
        w.wait_send()

    @pl.when(b_on)
    def _():
        wait_bytes(br.at[pl.ds(0, HALF_JOINT - 1)], ssem.at[5])
        wait_bytes(mb.at[pl.ds(0, CHIPS - 1)], ssem.at[6])

    @pl.when(jnp.logical_not(b_on))
    def _():
        wait_bytes(br.at[pl.ds(0, HALF_JOINT)], ssem.at[5])

    @pl.when(c_on)
    def _():
        wait_bytes(cr.at[pl.ds(0, HALF_HEADS - 1)], ssem.at[8])
        wait_bytes(dummy, ssem.at[9])

    @pl.when(jnp.logical_not(c_on))
    def _():
        wait_bytes(cr.at[pl.ds(0, HALF_HEADS)], ssem.at[8])


def body(
    token_ids, lengths, embed_table, attn_gain, w_qkv, qkv_bias, cache_keys, cache_values, w_out,
    mlp_gain, w_gate, w_up, w_down,
):
    steps, prompts = token_ids.shape
    vocab_rows, model = embed_table.shape
    span = cache_keys.shape[1]
    width = w_out.shape[1]
    block = PLANE * width
    per_group = HEADS // KV_HEADS
    half = HEAD_DIM // 2
    frequency = np.float32(ROPE_BASE) ** (
        np.float32(-2.0) * np.arange(half, dtype=np.float32) / np.float32(HEAD_DIM)
    )
    frequency = jnp.asarray(np.tile(np.concatenate([frequency, frequency]), (ROWS, 1)), F32)
    vmem = pl.BlockSpec(memory_space=pltpu.VMEM)
    smem = pl.BlockSpec(memory_space=pltpu.SMEM)
    hbm = pl.BlockSpec(memory_space=pl.ANY)
    w_out_t = w_out.T

    def like(a):
        return pltpu.VMEM(a.shape, a.dtype)

    def tile(*lead, dtype=F32):
        return pltpu.VMEM((*lead, ROWS, LANES), dtype)

    def wide(*lead, dtype):
        return pltpu.VMEM((*lead, ROWS, block), dtype)

    attended, layer_out = pl.pallas_call(
        kernel,
        out_shape=(
            jax.ShapeDtypeStruct((ROWS, HEADS * HEAD_DIM), BF16),
            jax.ShapeDtypeStruct((ROWS, width), BF16),
        ),
        in_specs=[smem, smem, vmem, hbm, vmem, hbm, vmem, hbm, hbm, hbm, vmem, hbm, hbm, hbm],
        out_specs=(vmem, vmem),
        scratch_shapes=[
            pltpu.VMEM((XS, vocab_rows, block), BF16),
            pltpu.VMEM((CORES, width, HALF_JOINT * LANES), BF16),
            pltpu.VMEM((CORES, prompts, span, GROUPS * LANES), BF16),
            pltpu.VMEM((CORES, prompts, span, GROUPS * LANES), BF16),
            pltpu.VMEM((CORES, width, model), BF16),
            pltpu.VMEM((model, 2 * LANES), BF16), pltpu.VMEM((XS, LANES, block), BF16),
            wide(XS, dtype=BF16), wide(XS - 1, dtype=BF16), tile(), tile(XS - 1),
            tile(YS), tile(PLANE - 1), tile(), tile(),
            tile(GROUPS, UNITS), tile(CHIPS - 1),
            pltpu.VMEM((ROWS, HALF_JOINT * LANES), BF16),
            pltpu.VMEM((GROUPS, per_group, 2 * ROWS, LANES), BF16),
            pltpu.VMEM((CHIPS - 1, 2 * ROWS, LANES), BF16), tile(CHIPS + 1),
            pltpu.VMEM((ROWS, HEADS * LANES), BF16),
            tile(), tile(CHIPS, dtype=BF16),
            pltpu.VMEM((ROWS, model), BF16),
            wide(XS, dtype=BF16), wide(XS - 1, dtype=BF16),
            tile(PLANE, dtype=BF16), tile(PLANE - 1, dtype=BF16),
            tile(GROUP - 1, dtype=BF16),
            pltpu.SemaphoreType.DMA((XS,)),
            pltpu.SemaphoreType.DMA((8 + XS,)),
            pltpu.SemaphoreType.DMA((14,)),
            pltpu.SemaphoreType.DMA((14,)),
            pltpu.SemaphoreType.DMA((GROUPS,)),
            pltpu.SemaphoreType.DMA((6,)),
            pltpu.SemaphoreType.DMA((6,)),
        ],
        compiler_params=pltpu.CompilerParams(
            collective_id=0, has_side_effects=True, vmem_limit_bytes=60 * 2**20
        ),
        name="layer",
    )(
        token_ids.T, lengths, frequency, embed_table, attn_gain.reshape(-1, LANES), w_qkv,
        qkv_bias.reshape(-1, LANES), cache_keys, cache_values, w_out_t,
        mlp_gain.reshape(-1, LANES), w_gate, w_up, w_down,
    )
    return (
        attended.reshape(steps, prompts, -1),
        layer_out.reshape(steps, prompts, width),
    )


def solution(mesh):
    return jax.shard_map(
        body,
        mesh=mesh,
        in_specs=(
            P(None, "parts"), P("parts"), P("seq", None), P(), P("seq", None), P(),
            P("parts", "seq", None), P("parts", "seq", None), P(None, "seq"), P(),
            P(None, "seq"), P(None, "seq"), P("seq", None),
        ),
        out_specs=(P(None, "parts", None), P(None, "parts", "seq")),
        check_vma=False,
    )
```

```python
import functools
import math

import jax
import jax.numpy as jnp
import numpy as np
from jax import lax
from jax.experimental import pallas as pl
from jax.experimental.pallas import tpu as pltpu
from jax.sharding import PartitionSpec as P

HEADS = 40
KV_HEADS = 8
HEAD_DIM = 128
NORM_EPS = 1e-06
ROPE_BASE = 1000000.0
MASKED = -1e30

ROWS = 8
LANES = 128
XS, YS, CORES = 8, 8, 2
PLANE = YS * CORES
CHIPS = XS * YS
GROUP = CHIPS * CORES
JOINT_HEADS = HEADS + 2 * KV_HEADS
HALF_JOINT = JOINT_HEADS // CORES
GROUPS = KV_HEADS // CORES
UNITS = JOINT_HEADS // KV_HEADS
JOINT_AT = (0, 2, 4, 6, 9, 11, 13)
HEAD_AT = (4, 6, 0, 2, 13)
FAR_FIRST = (4, 3, 5, 2, 6, 1, 7, 0)
HALF_HEADS = HEADS // CORES
MESH = pl.DeviceIdType.MESH
F32, BF16 = jnp.float32, jnp.bfloat16


def position(within, places):
    at, ok = 0, False
    for r, p in enumerate(places):
        at = jnp.where(within == p, r, at)
        ok = jnp.logical_or(ok, within == p)
    return at, ok


def own_gain(gain, me, width):
    start = me * width
    tile, off = lax.div(start, LANES), lax.rem(start, LANES)
    line = lax.broadcasted_iota(jnp.int32, gain.shape, 0)
    lane = lax.broadcasted_iota(jnp.int32, (1, LANES), 1)
    first = jnp.sum(jnp.where(line == tile, gain, 0.0), axis=0, keepdims=True)
    second = jnp.sum(jnp.where(line == tile + 1, gain, 0.0), axis=0, keepdims=True)
    both = jnp.where(lane >= off, first, second)
    return pltpu.roll(jnp.broadcast_to(both, (ROWS, LANES)), lax.rem(LANES - off, LANES), 1)


def lanes_of(n):
    return pl.ds(pl.multiple_of(n * LANES, LANES), LANES)


def send(src, dst, send_sem, recv_sem, device):
    copy = pltpu.make_async_remote_copy(
        src_ref=src,
        dst_ref=dst,
        send_sem=send_sem,
        recv_sem=recv_sem,
        device_id={"seq": device},
        device_id_type=MESH,
    )
    copy.start()


def split_level(level):
    lane = lax.broadcasted_iota(jnp.int32, level.shape, 1)
    first = level.astype(BF16).astype(F32)
    second = (level - first).astype(BF16).astype(F32)
    third = level - first - second
    quarter = LANES // 4
    return jnp.where(
        lane < quarter, first,
        jnp.where(lane < 2 * quarter, second, jnp.where(lane < 3 * quarter, third, 0.0)),
    )


def join_level(parts):
    level = parts + pltpu.roll(parts, LANES // 2, 1)
    return level + pltpu.roll(level, LANES // 4, 1)


def packed(value, level):
    return jnp.concatenate([value, split_level(level)], axis=0).astype(BF16)


def wait_bytes(ref, sem):
    pltpu.make_async_copy(ref, ref, sem).wait()


def cut_pieces(tiles, width, count):
    lane = lax.broadcasted_iota(jnp.int32, (ROWS, LANES), 1)
    pieces = []
    for j in range(count):
        t, off = divmod(width * j, LANES)
        piece = tiles[t] if off == 0 else pltpu.roll(tiles[t], LANES - off, 1)
        if off + width > LANES:
            rest = pltpu.roll(tiles[t + 1], LANES - off, 1)
            piece = jnp.where(lane < LANES - off, piece, rest)
        pieces.append(piece)
    return pieces


def join_pieces(pieces, width, tiles):
    lane = lax.broadcasted_iota(jnp.int32, (ROWS, LANES), 1)
    out = [None] * tiles

    def put(t, value):
        out[t] = value if out[t] is None else out[t] + value

    for j, piece in enumerate(pieces):
        t, off = divmod(width * j, LANES)
        moved = piece if off == 0 else pltpu.roll(piece, off, 1)
        if off + width > LANES:
            put(t, jnp.where(lane >= off, moved, 0.0))
            put(t + 1, jnp.where(lane < off, moved, 0.0))
        else:
            put(t, moved)
    return out


def kernel(
    ids_ref, len_ref, freq_ref, table_hbm, gain_ref, wqkv_hbm, bias_ref, keys_hbm, values_hbm,
    wout_hbm, mgain_ref, wgate_hbm, wup_hbm, wdown_hbm,
    att_ref, lay_ref,
    table, wqkv, keys, values, wout, wgu, wdown,
    a1s, a1r, a2s, a2r, cosr, sinr,
    bs, br, jflat,
    cs, cr, levels, aflat, tmp, mb, nflat,
    es, er, e2s, e2r, dummy,
    tsem, wsem, ssem, rsem, jsem, osem, psem,
):
    me = lax.axis_index("seq")
    x = lax.div(me, PLANE)
    j0 = lax.rem(me, PLANE)
    y = lax.div(j0, CORES)
    chip = lax.div(me, CORES)
    c = lax.rem(me, CORES)
    other = me + 1 - 2 * c
    width = lay_ref.shape[1]
    block = PLANE * width
    tiles = block // LANES
    vocab_rows = table.shape[1]
    group = HEADS // KV_HEADS

    x_peers = [(k, lax.rem(x + k, XS)) for k in FAR_FIRST[:-1]]
    y_part = [lax.rem(y + k, YS) * CORES for k in range(YS)]
    x_part = [lax.rem(x + k, XS) * PLANE for k in range(XS)]
    plane_peers = [
        (k, e, y_part[k] + lax.rem(c + e, CORES))
        for k in FAR_FIRST for e in range(CORES) if k or e
    ]
    chip_peers = sorted(
        [(i, j) for i in range(XS) for j in range(YS) if i or j],
        key=lambda p: -min(p[0], XS - p[0]) - min(p[1], YS - p[1]),
    )

    def to_all(tile, send_sem, recv_sem):
        for i, j in chip_peers:
            for e in range(CORES):
                send(tile, tile, send_sem, recv_sem, x_part[i] + y_part[j] + e)
        send(tile, tile, send_sem, recv_sem, other)

    def to_core(tile, send_sem, recv_sem):
        for i, j in chip_peers:
            send(tile, tile, send_sem, recv_sem, x_part[i] + y_part[j] + c)

    barrier = pltpu.get_barrier_semaphore()
    for _, p in x_peers:
        pl.semaphore_signal(barrier, inc=1, device_id={"seq": p * PLANE + j0}, device_id_type=MESH)
    order = [p for _, p in x_peers] + [x]
    blocks = [pl.ds(pl.multiple_of(p * block, LANES), block) for p in order]
    loads = []
    for k, at in enumerate(blocks):
        loads.append(pltpu.make_async_copy(table_hbm.at[:, at], table.at[k], tsem.at[k]))
        loads[-1].start()
    for _, _, p in plane_peers:
        pl.semaphore_signal(barrier, inc=1, device_id={"seq": x * PLANE + p}, device_id_type=MESH)

    def parts(side):
        def cols(start, n):
            return pl.ds(pl.multiple_of(start * LANES, LANES), n * LANES)

        out = []
        for at, n, to in (
            (HALF_HEADS * side, HALF_HEADS, 0),
            (HEADS + GROUPS * side, GROUPS, HALF_HEADS),
            (HEADS + KV_HEADS + GROUPS * side, GROUPS, HALF_HEADS + GROUPS),
        ):
            out.append((wqkv_hbm.at[:, cols(at, n)], wqkv.at[c, :, cols(to, n)]))
        mine = cols(GROUPS * side, GROUPS)
        out.append((keys_hbm.at[:, :, mine], keys.at[c]))
        out.append((values_hbm.at[:, :, mine], values.at[c]))
        out.append((wout_hbm, wout.at[c]))
        return out

    weights = [
        pltpu.make_async_copy(src, dst, wsem.at[k])
        for k, (src, dst) in enumerate(
            parts(c) + [(wgate_hbm, wgu.at[:, :LANES]), (wup_hbm, wgu.at[:, LANES:])]
            + [(wdown_hbm.at[:, at], wdown.at[k]) for k, at in enumerate(blocks)]
        )
    ]
    for w in weights:
        w.start()
    swaps = [
        pltpu.make_async_remote_copy(
            src_ref=src, dst_ref=dst, send_sem=osem.at[k], recv_sem=psem.at[k],
            device_id={"seq": other}, device_id_type=MESH,
        )
        for k, (src, dst) in enumerate(parts(1 - c))
    ]

    lane = lax.broadcasted_iota(jnp.int32, (ROWS, LANES), 1)
    row = lax.broadcasted_iota(jnp.int32, (ROWS, LANES), 0)
    low = lane < LANES // 2
    prompts = len_ref.shape[0]

    local = jnp.full((ROWS, vocab_rows), -1, jnp.int32)
    vrow = lax.broadcasted_iota(jnp.int32, (ROWS, vocab_rows), 0)
    vcol = lax.broadcasted_iota(jnp.int32, (ROWS, vocab_rows), 1)
    for r in range(ROWS):
        local = jnp.where(vrow == r, ids_ref[r % prompts, r // prompts] - me * vocab_rows, local)
    chosen = jnp.where(local == vcol, 1.0, 0.0).astype(BF16)
    square = jnp.zeros((ROWS, LANES), F32)
    for k in range(XS):
        loads[k].wait()
        found = jnp.dot(chosen, table[k], preferred_element_type=F32)
        a1s[k, :, :block] = found.astype(BF16)
        for t in range(tiles):
            v = found[:, t * LANES : (t + 1) * LANES]
            square = square + v * v
    square = split_level(
        jnp.broadcast_to(jnp.sum(square, axis=-1, keepdims=True) / (XS * block), (ROWS, LANES))
    ).astype(BF16)
    for k in range(XS):
        a1s[k, :, block:] = square
    pl.semaphore_wait(barrier, XS + PLANE - 2)
    for k, (d, p) in enumerate(x_peers):
        send(a1s.at[k], a1r.at[d - 1], ssem.at[0], rsem.at[0], p * PLANE + j0)
    for w in swaps:
        w.start()

    place = jnp.zeros((ROWS, LANES), jnp.int32)
    for r in range(ROWS):
        place = jnp.where(row == r, len_ref[r % prompts] + r // prompts, place)
    angle = place.astype(F32) * freq_ref[...]
    cosr[...] = jnp.cos(angle)
    sine = jnp.sin(angle)
    sinr[...] = jnp.where(lane < HEAD_DIM // 2, -sine, sine)

    wait_bytes(a1r, rsem.at[0])
    total = a1s[XS - 1].astype(F32)
    for k in range(XS - 1):
        total = total + a1r[k].astype(F32)
    found = [total[:, t * LANES : (t + 1) * LANES] for t in range(tiles)]
    square = join_level(total[:, block:])
    pair = CORES * width
    for j, piece in enumerate(cut_pieces(found, pair, YS)):
        a2s[j] = jnp.where(lane < pair, piece, square)
    for k, e, p in plane_peers:
        to = lax.div(p, CORES)
        send(a2s.at[to], a2r.at[k * CORES + e - 1], ssem.at[2], rsem.at[2], x * PLANE + p)
    gain = own_gain(gain_ref[...].astype(F32), chip, pair)
    for k in range(3):
        weights[k].wait()
        swaps[k].wait_recv()
    wait_bytes(a2r, rsem.at[2])
    stream = a2s[y] + jnp.sum(a2r[...], axis=0)
    scale = lax.rsqrt(jnp.broadcast_to(stream[:, LANES - 1 :], (ROWS, LANES)) + NORM_EPS)
    normed = stream * scale * gain
    normed = [
        v[:, :width].astype(BF16) for v in (normed, pltpu.roll(normed, LANES - width, 1))
    ]

    half_group = lax.div(chip, CHIPS // GROUPS)
    within = lax.rem(chip, CHIPS // GROUPS)
    far_groups = [lax.rem(half_group + k, GROUPS) for k in (2, 1, 3, 0)]
    near_groups = [lax.rem(half_group + k, GROUPS) for k in (0, 1, 3, 2)]

    def project(at, n):
        cols = pl.ds(pl.multiple_of(at * LANES, LANES), n * LANES)
        got = sum(
            jnp.dot(normed[e], wqkv[e, :, cols], preferred_element_type=F32) for e in range(CORES)
        )
        return [got[:, t * LANES : (t + 1) * LANES] for t in range(n)]

    for n, g in enumerate(far_groups):
        mine = (
            project(group * g, group) + project(HALF_HEADS + g, 1)
            + project(HALF_HEADS + GROUPS + g, 1)
        )
        for r in range(UNITS):
            bs[n, r] = mine[r]
        for r in range(UNITS):
            p = (CHIPS // GROUPS) * g + JOINT_AT[r]

            def go(n=n, r=r, p=p):
                slot = lax.rem(chip - p + CHIPS, CHIPS) - 1
                send(bs.at[n, r], br.at[slot], ssem.at[5], rsem.at[5], p * CORES + c)

            if n < GROUPS - 1:
                go()
            else:
                pl.when(within != JOINT_AT[r])(go)

    rb, b_on = position(within, JOINT_AT)
    nb = UNITS * half_group + rb

    @pl.when(b_on)
    def _():
        wait_bytes(br, rsem.at[5])
        at = jnp.where(
            rb < group, HALF_HEADS * c + group * half_group + rb,
            HEADS + GROUPS * c + half_group + jnp.where(rb > group, KV_HEADS, 0),
        )
        total = bs[GROUPS - 1, rb].astype(F32)
        for k in range(CHIPS - 1):
            total = total + br[k].astype(F32)
        total = total + bias_ref[pl.ds(at, 1), :]
        joint = total.astype(BF16).astype(F32)
        turned = joint * cosr[...] + pltpu.roll(joint, HEAD_DIM // 2, 1) * sinr[...]
        turn = jnp.where(rb <= group, 1.0, 0.0)
        jflat[:, lanes_of(nb)] = jnp.where(turn > 0.5, turned, joint).astype(BF16)
        tile = jflat.at[:, lanes_of(nb)]
        to_core(tile, ssem.at[6], jsem.at[half_group])

    for k in range(3, 5):
        weights[k].wait()
        swaps[k].wait_recv()
    span = keys.shape[2]
    lines = group * ROWS
    wide_row = lax.broadcasted_iota(jnp.int32, (lines, CORES * span), 0)
    even = lax.rem(wide_row, prompts) == 0
    where = chip * (CORES * span) + lax.broadcasted_iota(jnp.int32, (lines, CORES * span), 1)
    valid = where < jnp.where(even, len_ref[0], len_ref[1])
    score_scale = 1.0 / math.sqrt(HEAD_DIM)
    nt = (((1,), (1,)), ((), ()))

    def joint_group(g, n=UNITS):
        return jflat.at[:, pl.ds(pl.multiple_of(g * UNITS * LANES, LANES), n * LANES)]

    for n, g in enumerate(near_groups):
        if n == 0:
            @pl.when(b_on)
            def _(g=g):
                wait_bytes(joint_group(g, UNITS - 1), jsem.at[g])

            @pl.when(jnp.logical_not(b_on))
            def _(g=g):
                wait_bytes(joint_group(g), jsem.at[g])
        else:
            wait_bytes(joint_group(g), jsem.at[g])
        at = lanes_of(g)
        query = jnp.concatenate(
            [jflat[:, lanes_of(UNITS * g + r)].astype(F32) for r in range(group)], axis=0
        ).astype(BF16)
        score = [
            jnp.concatenate(
                [
                    lax.dot_general(query, keys[e, b, :, at], nt, preferred_element_type=F32)
                    for e in range(CORES)
                ],
                axis=1,
            )
            for b in range(prompts)
        ]
        score = jnp.where(valid, jnp.where(even, score[0], score[1]) * score_scale, MASKED)
        top = jnp.max(score, axis=-1, keepdims=True)
        weight = jnp.where(valid, jnp.exp(score - top), 0.0)
        total = jnp.sum(weight, axis=-1, keepdims=True)
        split = [
            jnp.where(even, weight, 0.0).astype(BF16), jnp.where(even, 0.0, weight).astype(BF16)
        ]
        summed = sum(
            jnp.dot(
                split[b][:, e * span : (e + 1) * span], values[e, b, :, at],
                preferred_element_type=F32,
            )
            for b in range(prompts)
            for e in range(CORES)
        )
        some = total > 0.0
        total = jnp.where(some, total, 1.0)
        level = jnp.broadcast_to(
            jnp.where(some, top + jnp.log(total), MASKED), (lines, LANES)
        )
        summed = summed / total
        for r in range(group):
            own = slice(r * ROWS, (r + 1) * ROWS)
            cs[n, r] = packed(summed[own], level[own])
        across = lax.rem(g + GROUPS // 2, GROUPS)
        for r in range(group):
            p = (CHIPS // GROUPS) * across + HEAD_AT[r]

            def go(n=n, r=r, p=p):
                slot = lax.rem(chip - p + CHIPS, CHIPS) - 1
                send(cs.at[n, r], cr.at[slot], ssem.at[8], rsem.at[8], p * CORES + c)

            if n < GROUPS - 1:
                go()
            else:
                pl.when(within != HEAD_AT[r])(go)

    rc, c_on = position(within, HEAD_AT)
    gc = lax.rem(half_group + GROUPS // 2, GROUPS)
    hc = HALF_HEADS * c + group * gc + rc

    @pl.when(c_on)
    def _():
        base = UNITS * gc
        query = jflat[:, lanes_of(base + rc)]
        new_key = jflat[:, lanes_of(base + group)]
        new_value = jflat[:, lanes_of(base + group + 1)]
        small_r = lax.broadcasted_iota(jnp.int32, (ROWS, ROWS), 0)
        small_c = lax.broadcasted_iota(jnp.int32, (ROWS, ROWS), 1)
        seen = jnp.logical_and(
            small_c <= small_r, lax.rem(small_c, prompts) == lax.rem(small_r, prompts)
        )
        score = lax.dot_general(query, new_key, nt, preferred_element_type=F32) * score_scale
        score = jnp.where(seen, score, MASKED)
        top = jnp.max(score, axis=-1, keepdims=True)
        weight = jnp.where(seen, jnp.exp(score - top), 0.0)
        total = jnp.sum(weight, axis=-1, keepdims=True)
        new_sum = jnp.dot(weight.astype(BF16), new_value, preferred_element_type=F32)
        best = top + jnp.log(total)
        levels[CHIPS] = jnp.broadcast_to(best, (ROWS, LANES))
        best = levels[CHIPS]
        wait_bytes(cr, rsem.at[8])

        def partial(s):
            return cs[GROUPS - 1, rc] if s == CHIPS - 1 else cr[s]

        for s in range(CHIPS):
            level = join_level(partial(s)[ROWS:].astype(F32))
            levels[s] = level
            best = jnp.maximum(best, level)
        den = jnp.exp(levels[CHIPS] - best)
        acc = new_sum / total * den
        for s in range(CHIPS):
            scale = jnp.exp(levels[s] - best)
            acc = acc + partial(s)[:ROWS].astype(F32) * scale
            den = den + scale
        aflat[:, lanes_of(hc)] = (acc / den).astype(BF16)
        to_all(aflat.at[:, lanes_of(hc)], ssem.at[9], rsem.at[9])
        wait_bytes(aflat.at[:, : (HEADS - 1) * LANES], rsem.at[9])

    @pl.when(jnp.logical_not(c_on))
    def _():
        wait_bytes(aflat, rsem.at[9])

    weights[5].wait()
    swaps[5].wait_recv()
    attended = aflat[...]
    tmp[...] = jnp.zeros((ROWS, LANES), F32)
    for e in range(CORES):
        tmp[:, e * width : (e + 1) * width] = lax.dot_general(
            attended, wout[e], nt, preferred_element_type=F32
        )
    mid = jnp.where(lane < pair, tmp[...] + stream, 0.0)
    mb[chip] = mid.astype(BF16)
    to_core(mb.at[chip], ssem.at[11], rsem.at[11])

    att_ref[...] = attended
    for w in weights[6:]:
        w.wait()
    wait_bytes(mb.at[pl.ds(0, CHIPS - 1)], rsem.at[11])
    mids = join_pieces([mb[p].astype(F32) for p in range(CHIPS)], pair, XS * tiles)
    square = jnp.zeros((ROWS, LANES), F32)
    for v in mids:
        square = square + v * v
    scale = lax.rsqrt(jnp.sum(square, axis=-1, keepdims=True) / (XS * block) + NORM_EPS)
    gain = mgain_ref[...].astype(F32)
    for g, v in enumerate(mids):
        nflat[:, g * LANES : (g + 1) * LANES] = (v * scale * gain[g : g + 1, :]).astype(BF16)
    normed_mid = nflat[...]
    both = jnp.dot(normed_mid, wgu[...], preferred_element_type=F32)
    gate, upper = both[:, :LANES], both[:, LANES:]
    hidden = (gate / (1.0 + jnp.exp(-gate)) * upper).astype(BF16)
    for batch in (range(XS // 2), range(XS // 2, XS)):
        for k in batch:
            es[k] = jnp.dot(hidden, wdown[k], preferred_element_type=F32).astype(BF16)
        for k in batch:
            if k < XS - 1:
                d, p = x_peers[k]
                send(es.at[k], er.at[d - 1], ssem.at[12], rsem.at[12], p * PLANE + j0)
    wait_bytes(er, rsem.at[12])
    total = es[XS - 1].astype(F32)
    for k in range(XS - 1):
        total = total + er[k].astype(F32)
    found = [total[:, t * LANES : (t + 1) * LANES] for t in range(tiles)]
    for j, piece in enumerate(cut_pieces(found, width, PLANE)):
        e2s[j] = piece.astype(BF16)
    for k, e, p in plane_peers:
        send(e2s.at[p], e2r.at[k * CORES + e - 1], ssem.at[13], rsem.at[13], x * PLANE + p)
    wait_bytes(e2r, rsem.at[13])
    final = e2s[j0].astype(F32)
    for k in range(PLANE - 1):
        final = final + e2r[k].astype(F32)
    final = final + jnp.where(row * 0 + c == 0, mid, pltpu.roll(mid, LANES - width, 1))
    lay_ref[...] = final[:, :width].astype(BF16)

    for sem, ref in (
        (0, a1r), (2, a2r), (12, er), (13, e2r),
    ):
        wait_bytes(ref, ssem.at[sem])
    wait_bytes(mb.at[pl.ds(0, CHIPS - 1)], ssem.at[11])
    for w in swaps:
        w.wait_send()

    @pl.when(b_on)
    def _():
        wait_bytes(br.at[pl.ds(0, HALF_JOINT - 1)], ssem.at[5])
        wait_bytes(mb.at[pl.ds(0, CHIPS - 1)], ssem.at[6])

    @pl.when(jnp.logical_not(b_on))
    def _():
        wait_bytes(br.at[pl.ds(0, HALF_JOINT)], ssem.at[5])

    @pl.when(c_on)
    def _():
        wait_bytes(cr.at[pl.ds(0, HALF_HEADS - 1)], ssem.at[8])
        wait_bytes(dummy, ssem.at[9])

    @pl.when(jnp.logical_not(c_on))
    def _():
        wait_bytes(cr.at[pl.ds(0, HALF_HEADS)], ssem.at[8])


def body(
    token_ids, lengths, embed_table, attn_gain, w_qkv, qkv_bias, cache_keys, cache_values, w_out,
    mlp_gain, w_gate, w_up, w_down,
):
    steps, prompts = token_ids.shape
    vocab_rows, model = embed_table.shape
    span = cache_keys.shape[1]
    width = w_out.shape[1]
    block = PLANE * width
    per_group = HEADS // KV_HEADS
    half = HEAD_DIM // 2
    frequency = np.float32(ROPE_BASE) ** (
        np.float32(-2.0) * np.arange(half, dtype=np.float32) / np.float32(HEAD_DIM)
    )
    frequency = jnp.asarray(np.tile(np.concatenate([frequency, frequency]), (ROWS, 1)), F32)
    vmem = pl.BlockSpec(memory_space=pltpu.VMEM)
    smem = pl.BlockSpec(memory_space=pltpu.SMEM)
    hbm = pl.BlockSpec(memory_space=pl.ANY)
    w_out_t = w_out.T

    def like(a):
        return pltpu.VMEM(a.shape, a.dtype)

    def tile(*lead, dtype=F32):
        return pltpu.VMEM((*lead, ROWS, LANES), dtype)

    def wide(*lead, dtype):
        return pltpu.VMEM((*lead, ROWS, block), dtype)

    def wider(*lead):
        return pltpu.VMEM((*lead, ROWS, block + LANES), BF16)

    attended, layer_out = pl.pallas_call(
        kernel,
        out_shape=(
            pltpu.VMEM((ROWS, HEADS * HEAD_DIM), BF16),
            pltpu.VMEM((ROWS, width), BF16),
        ),
        in_specs=[smem, smem, vmem, hbm, vmem, hbm, vmem, hbm, hbm, hbm, vmem, hbm, hbm, hbm],
        out_specs=(vmem, vmem),
        scratch_shapes=[
            pltpu.VMEM((XS, vocab_rows, block), BF16),
            pltpu.VMEM((CORES, width, HALF_JOINT * LANES), BF16),
            pltpu.VMEM((CORES, prompts, span, GROUPS * LANES), BF16),
            pltpu.VMEM((CORES, prompts, span, GROUPS * LANES), BF16),
            pltpu.VMEM((CORES, width, model), BF16),
            pltpu.VMEM((model, 2 * LANES), BF16), pltpu.VMEM((XS, LANES, block), BF16),
            wider(XS), wider(XS - 1),
            tile(YS), tile(PLANE - 1), tile(), tile(),
            tile(GROUPS, UNITS), tile(CHIPS - 1),
            pltpu.VMEM((ROWS, HALF_JOINT * LANES), BF16),
            pltpu.VMEM((GROUPS, per_group, 2 * ROWS, LANES), BF16),
            pltpu.VMEM((CHIPS - 1, 2 * ROWS, LANES), BF16), tile(CHIPS + 1),
            pltpu.VMEM((ROWS, HEADS * LANES), BF16),
            tile(), tile(CHIPS, dtype=BF16),
            pltpu.VMEM((ROWS, model), BF16),
            wide(XS, dtype=BF16), wide(XS - 1, dtype=BF16),
            tile(PLANE, dtype=BF16), tile(PLANE - 1, dtype=BF16),
            tile(GROUP - 1, dtype=BF16),
            pltpu.SemaphoreType.DMA((XS,)),
            pltpu.SemaphoreType.DMA((8 + XS,)),
            pltpu.SemaphoreType.DMA((14,)),
            pltpu.SemaphoreType.DMA((14,)),
            pltpu.SemaphoreType.DMA((GROUPS,)),
            pltpu.SemaphoreType.DMA((6,)),
            pltpu.SemaphoreType.DMA((6,)),
        ],
        compiler_params=pltpu.CompilerParams(
            collective_id=0, has_side_effects=True, vmem_limit_bytes=60 * 2**20
        ),
        name="layer",
    )(
        token_ids.T, lengths, frequency, embed_table, attn_gain.reshape(-1, LANES), w_qkv,
        qkv_bias.reshape(-1, LANES), cache_keys, cache_values, w_out_t,
        mlp_gain.reshape(-1, LANES), w_gate, w_up, w_down,
    )
    return pl.pallas_call(
        finish,
        out_shape=(
            jax.ShapeDtypeStruct((steps, prompts, HEADS * HEAD_DIM), BF16),
            jax.ShapeDtypeStruct((steps, prompts, width), BF16),
        ),
        in_specs=[vmem, vmem],
        out_specs=(vmem, vmem),
        name="finish",
    )(
        pltpu.with_memory_space_constraint(attended, pltpu.VMEM),
        pltpu.with_memory_space_constraint(layer_out, pltpu.VMEM),
    )


def finish(att_ref, lay_ref, att_out, lay_out):
    n = att_out.shape[1]
    for k in range(att_out.shape[0]):
        att_out[k] = att_ref[k * n : (k + 1) * n]
        lay_out[k] = lay_ref[k * n : (k + 1) * n]


def solution(mesh):
    return jax.shard_map(
        body,
        mesh=mesh,
        in_specs=(
            P(None, "parts"), P("parts"), P("seq", None), P(), P("seq", None), P(),
            P("parts", "seq", None), P("parts", "seq", None), P(None, "seq"), P(),
            P(None, "seq"), P(None, "seq"), P("seq", None),
        ),
        out_specs=(P(None, "parts", None), P(None, "parts", "seq")),
        check_vma=False,
    )
```

```python
import functools
import math

import jax
import jax.numpy as jnp
import numpy as np
from jax import lax
from jax.experimental import pallas as pl
from jax.experimental.pallas import tpu as pltpu
from jax.sharding import PartitionSpec as P

HEADS = 40
KV_HEADS = 8
HEAD_DIM = 128
NORM_EPS = 1e-06
ROPE_BASE = 1000000.0
MASKED = -1e30

ROWS = 8
LANES = 128
XS, YS, CORES = 8, 8, 2
PLANE = YS * CORES
CHIPS = XS * YS
GROUP = CHIPS * CORES
JOINT_HEADS = HEADS + 2 * KV_HEADS
HALF_JOINT = JOINT_HEADS // CORES
GROUPS = KV_HEADS // CORES
UNITS = JOINT_HEADS // KV_HEADS
JOINT_AT = (0, 2, 4, 6, 9, 11, 13)
HEAD_AT = (4, 6, 0, 2, 13)
FAR_FIRST = (4, 3, 5, 2, 6, 1, 7, 0)
HALF_HEADS = HEADS // CORES
MESH = pl.DeviceIdType.MESH
F32, BF16 = jnp.float32, jnp.bfloat16


def position(within, places):
    at, ok = 0, False
    for r, p in enumerate(places):
        at = jnp.where(within == p, r, at)
        ok = jnp.logical_or(ok, within == p)
    return at, ok


def own_gain(gain, me, width):
    start = me * width
    tile, off = lax.div(start, LANES), lax.rem(start, LANES)
    line = lax.broadcasted_iota(jnp.int32, gain.shape, 0)
    lane = lax.broadcasted_iota(jnp.int32, (1, LANES), 1)
    first = jnp.sum(jnp.where(line == tile, gain, 0.0), axis=0, keepdims=True)
    second = jnp.sum(jnp.where(line == tile + 1, gain, 0.0), axis=0, keepdims=True)
    both = jnp.where(lane >= off, first, second)
    return pltpu.roll(jnp.broadcast_to(both, (ROWS, LANES)), lax.rem(LANES - off, LANES), 1)


def lanes_of(n):
    return pl.ds(pl.multiple_of(n * LANES, LANES), LANES)


def send(src, dst, send_sem, recv_sem, device):
    copy = pltpu.make_async_remote_copy(
        src_ref=src,
        dst_ref=dst,
        send_sem=send_sem,
        recv_sem=recv_sem,
        device_id={"seq": device},
        device_id_type=MESH,
    )
    copy.start()


def split_level(level):
    lane = lax.broadcasted_iota(jnp.int32, level.shape, 1)
    first = level.astype(BF16).astype(F32)
    second = (level - first).astype(BF16).astype(F32)
    third = level - first - second
    quarter = LANES // 4
    return jnp.where(
        lane < quarter, first,
        jnp.where(lane < 2 * quarter, second, jnp.where(lane < 3 * quarter, third, 0.0)),
    )


def join_level(parts):
    level = parts + pltpu.roll(parts, LANES // 2, 1)
    return level + pltpu.roll(level, LANES // 4, 1)


def packed(value, level):
    return jnp.concatenate([value, split_level(level)], axis=0).astype(BF16)


def wait_bytes(ref, sem):
    pltpu.make_async_copy(ref, ref, sem).wait()


def cut_pieces(tiles, width, count):
    lane = lax.broadcasted_iota(jnp.int32, (ROWS, LANES), 1)
    pieces = []
    for j in range(count):
        t, off = divmod(width * j, LANES)
        piece = tiles[t] if off == 0 else pltpu.roll(tiles[t], LANES - off, 1)
        if off + width > LANES:
            rest = pltpu.roll(tiles[t + 1], LANES - off, 1)
            piece = jnp.where(lane < LANES - off, piece, rest)
        pieces.append(piece)
    return pieces


def join_pieces(pieces, width, tiles):
    lane = lax.broadcasted_iota(jnp.int32, (ROWS, LANES), 1)
    out = [None] * tiles

    def put(t, value):
        out[t] = value if out[t] is None else out[t] + value

    for j, piece in enumerate(pieces):
        t, off = divmod(width * j, LANES)
        moved = piece if off == 0 else pltpu.roll(piece, off, 1)
        if off + width > LANES:
            put(t, jnp.where(lane >= off, moved, 0.0))
            put(t + 1, jnp.where(lane < off, moved, 0.0))
        else:
            put(t, moved)
    return out


def kernel(
    ids_ref, len_ref, freq_ref, table_hbm, gain_ref, wqkv_hbm, bias_ref, keys_hbm, values_hbm,
    wout_hbm, mgain_ref, wgate_hbm, wup_hbm, wdown_hbm,
    att_ref, lay_ref,
    table, wqkv, keys, values, wout, wgu, wdown,
    a1s, a1r, a2s, a2r, cosr, sinr,
    bs, br, jflat,
    cs, cr, levels, aflat, tmp, mb, nflat,
    es, er, e2s, e2r, dummy,
    tsem, wsem, ssem, rsem, jsem, osem, psem,
):
    me = lax.axis_index("seq")
    x = lax.div(me, PLANE)
    j0 = lax.rem(me, PLANE)
    y = lax.div(j0, CORES)
    chip = lax.div(me, CORES)
    c = lax.rem(me, CORES)
    other = me + 1 - 2 * c
    width = lay_ref.shape[1]
    block = PLANE * width
    tiles = block // LANES
    vocab_rows = table.shape[1]
    group = HEADS // KV_HEADS

    x_peers = [(k, lax.rem(x + k, XS)) for k in FAR_FIRST[:-1]]
    y_part = [lax.rem(y + k, YS) * CORES for k in range(YS)]
    x_part = [lax.rem(x + k, XS) * PLANE for k in range(XS)]
    plane_peers = [
        (k, e, y_part[k] + lax.rem(c + e, CORES))
        for k in FAR_FIRST for e in range(CORES) if k or e
    ]
    chip_peers = sorted(
        [(i, j) for i in range(XS) for j in range(YS) if i or j],
        key=lambda p: -min(p[0], XS - p[0]) - min(p[1], YS - p[1]),
    )

    def to_all(tile, send_sem, recv_sem):
        for i, j in chip_peers:
            for e in range(CORES):
                send(tile, tile, send_sem, recv_sem, x_part[i] + y_part[j] + e)
        send(tile, tile, send_sem, recv_sem, other)

    def to_core(tile, send_sem, recv_sem):
        for i, j in chip_peers:
            send(tile, tile, send_sem, recv_sem, x_part[i] + y_part[j] + c)

    barrier = pltpu.get_barrier_semaphore()
    for _, p in x_peers:
        pl.semaphore_signal(barrier, inc=1, device_id={"seq": p * PLANE + j0}, device_id_type=MESH)
    order = [p for _, p in x_peers] + [x]
    blocks = [pl.ds(pl.multiple_of(p * block, LANES), block) for p in order]
    loads = []
    for k, at in enumerate(blocks):
        loads.append(pltpu.make_async_copy(table_hbm.at[:, at], table.at[k], tsem.at[k]))
        loads[-1].start()
    for _, _, p in plane_peers:
        pl.semaphore_signal(barrier, inc=1, device_id={"seq": x * PLANE + p}, device_id_type=MESH)

    def parts(side):
        def cols(start, n):
            return pl.ds(pl.multiple_of(start * LANES, LANES), n * LANES)

        out = []
        for at, n, to in (
            (HALF_HEADS * side, HALF_HEADS, 0),
            (HEADS + GROUPS * side, GROUPS, HALF_HEADS),
            (HEADS + KV_HEADS + GROUPS * side, GROUPS, HALF_HEADS + GROUPS),
        ):
            out.append((wqkv_hbm.at[:, cols(at, n)], wqkv.at[c, :, cols(to, n)]))
        mine = cols(GROUPS * side, GROUPS)
        out.append((keys_hbm.at[:, :, mine], keys.at[c]))
        out.append((values_hbm.at[:, :, mine], values.at[c]))
        out.append((wout_hbm, wout.at[c]))
        return out

    weights = [
        pltpu.make_async_copy(src, dst, wsem.at[k])
        for k, (src, dst) in enumerate(
            parts(c) + [(wgate_hbm, wgu.at[:, :LANES]), (wup_hbm, wgu.at[:, LANES:])]
            + [(wdown_hbm.at[:, at], wdown.at[k]) for k, at in enumerate(blocks)]
        )
    ]
    for w in weights:
        w.start()
    swaps = [
        pltpu.make_async_remote_copy(
            src_ref=src, dst_ref=dst, send_sem=osem.at[k], recv_sem=psem.at[k],
            device_id={"seq": other}, device_id_type=MESH,
        )
        for k, (src, dst) in enumerate(parts(1 - c))
    ]

    lane = lax.broadcasted_iota(jnp.int32, (ROWS, LANES), 1)
    row = lax.broadcasted_iota(jnp.int32, (ROWS, LANES), 0)
    low = lane < LANES // 2
    prompts = len_ref.shape[0]

    local = jnp.full((ROWS, vocab_rows), -1, jnp.int32)
    vrow = lax.broadcasted_iota(jnp.int32, (ROWS, vocab_rows), 0)
    vcol = lax.broadcasted_iota(jnp.int32, (ROWS, vocab_rows), 1)
    for r in range(ROWS):
        local = jnp.where(vrow == r, ids_ref[r % prompts, r // prompts] - me * vocab_rows, local)
    chosen = jnp.where(local == vcol, 1.0, 0.0).astype(BF16)
    square = jnp.zeros((ROWS, LANES), F32)
    for k in range(XS):
        loads[k].wait()
        found = jnp.dot(chosen, table[k], preferred_element_type=F32)
        a1s[k, :, :block] = found.astype(BF16)
        for t in range(tiles):
            v = found[:, t * LANES : (t + 1) * LANES]
            square = square + v * v
    square = split_level(
        jnp.broadcast_to(jnp.sum(square, axis=-1, keepdims=True) / (XS * block), (ROWS, LANES))
    ).astype(BF16)
    for k in range(XS):
        a1s[k, :, block:] = square
    pl.semaphore_wait(barrier, XS + PLANE - 2)
    for k, (d, p) in enumerate(x_peers):
        send(a1s.at[k], a1r.at[d - 1], ssem.at[0], rsem.at[0], p * PLANE + j0)
    for w in swaps:
        w.start()

    place = jnp.zeros((ROWS, LANES), jnp.int32)
    for r in range(ROWS):
        place = jnp.where(row == r, len_ref[r % prompts] + r // prompts, place)
    angle = place.astype(F32) * freq_ref[...]
    cosr[...] = jnp.cos(angle)
    sine = jnp.sin(angle)
    sinr[...] = jnp.where(lane < HEAD_DIM // 2, -sine, sine)

    wait_bytes(a1r, rsem.at[0])
    total = a1s[XS - 1].astype(F32)
    for k in range(XS - 1):
        total = total + a1r[k].astype(F32)
    found = [total[:, t * LANES : (t + 1) * LANES] for t in range(tiles)]
    square = join_level(total[:, block:])
    pair = CORES * width
    for j, piece in enumerate(cut_pieces(found, pair, YS)):
        a2s[j] = jnp.where(lane < pair, piece, square)
    for k, e, p in plane_peers:
        to = lax.div(p, CORES)
        send(a2s.at[to], a2r.at[k * CORES + e - 1], ssem.at[2], rsem.at[2], x * PLANE + p)
    gain = own_gain(gain_ref[...].astype(F32), chip, pair)
    for k in range(3):
        weights[k].wait()
        swaps[k].wait_recv()
    wait_bytes(a2r, rsem.at[2])
    stream = a2s[y] + jnp.sum(a2r[...], axis=0)
    scale = lax.rsqrt(jnp.broadcast_to(stream[:, LANES - 1 :], (ROWS, LANES)) + NORM_EPS)
    normed = stream * scale * gain
    normed = [
        v[:, :width].astype(BF16) for v in (normed, pltpu.roll(normed, LANES - width, 1))
    ]

    half_group = lax.div(chip, CHIPS // GROUPS)
    within = lax.rem(chip, CHIPS // GROUPS)
    far_groups = [lax.rem(half_group + k, GROUPS) for k in (2, 1, 3, 0)]
    near_groups = [lax.rem(half_group + k, GROUPS) for k in (0, 1, 3, 2)]

    def project(at, n):
        cols = pl.ds(pl.multiple_of(at * LANES, LANES), n * LANES)
        got = sum(
            jnp.dot(normed[e], wqkv[e, :, cols], preferred_element_type=F32) for e in range(CORES)
        )
        return [got[:, t * LANES : (t + 1) * LANES] for t in range(n)]

    for n, g in enumerate(far_groups):
        mine = (
            project(group * g, group) + project(HALF_HEADS + g, 1)
            + project(HALF_HEADS + GROUPS + g, 1)
        )
        for r in range(UNITS):
            bs[n, r] = mine[r]
        for r in range(UNITS):
            p = (CHIPS // GROUPS) * g + JOINT_AT[r]

            def go(n=n, r=r, p=p):
                slot = lax.rem(chip - p + CHIPS, CHIPS) - 1
                send(bs.at[n, r], br.at[slot], ssem.at[5], rsem.at[5], p * CORES + c)

            if n < GROUPS - 1:
                go()
            else:
                pl.when(within != JOINT_AT[r])(go)

    rb, b_on = position(within, JOINT_AT)
    nb = UNITS * half_group + rb

    @pl.when(b_on)
    def _():
        wait_bytes(br, rsem.at[5])
        at = jnp.where(
            rb < group, HALF_HEADS * c + group * half_group + rb,
            HEADS + GROUPS * c + half_group + jnp.where(rb > group, KV_HEADS, 0),
        )
        total = bs[GROUPS - 1, rb].astype(F32)
        for k in range(CHIPS - 1):
            total = total + br[k].astype(F32)
        total = total + bias_ref[pl.ds(at, 1), :]
        joint = total.astype(BF16).astype(F32)
        turned = joint * cosr[...] + pltpu.roll(joint, HEAD_DIM // 2, 1) * sinr[...]
        turn = jnp.where(rb <= group, 1.0, 0.0)
        jflat[:, lanes_of(nb)] = jnp.where(turn > 0.5, turned, joint).astype(BF16)
        tile = jflat.at[:, lanes_of(nb)]
        to_core(tile, ssem.at[6], jsem.at[half_group])

    for k in range(3, 5):
        weights[k].wait()
        swaps[k].wait_recv()
    span = keys.shape[2]
    lines = group * ROWS
    wide_row = lax.broadcasted_iota(jnp.int32, (lines, CORES * span), 0)
    even = lax.rem(wide_row, prompts) == 0
    where = chip * (CORES * span) + lax.broadcasted_iota(jnp.int32, (lines, CORES * span), 1)
    valid = where < jnp.where(even, len_ref[0], len_ref[1])
    score_scale = 1.0 / math.sqrt(HEAD_DIM)
    nt = (((1,), (1,)), ((), ()))

    def joint_group(g, n=UNITS):
        return jflat.at[:, pl.ds(pl.multiple_of(g * UNITS * LANES, LANES), n * LANES)]

    for n, g in enumerate(near_groups):
        if n == 0:
            @pl.when(b_on)
            def _(g=g):
                wait_bytes(joint_group(g, UNITS - 1), jsem.at[g])

            @pl.when(jnp.logical_not(b_on))
            def _(g=g):
                wait_bytes(joint_group(g), jsem.at[g])
        else:
            wait_bytes(joint_group(g), jsem.at[g])
        at = lanes_of(g)
        query = jnp.concatenate(
            [jflat[:, lanes_of(UNITS * g + r)].astype(F32) for r in range(group)], axis=0
        ).astype(BF16)
        score = [
            jnp.concatenate(
                [
                    lax.dot_general(query, keys[e, b, :, at], nt, preferred_element_type=F32)
                    for e in range(CORES)
                ],
                axis=1,
            )
            for b in range(prompts)
        ]
        score = jnp.where(valid, jnp.where(even, score[0], score[1]) * score_scale, MASKED)
        top = jnp.max(score, axis=-1, keepdims=True)
        weight = jnp.where(valid, jnp.exp(score - top), 0.0)
        total = jnp.sum(weight, axis=-1, keepdims=True)
        split = [
            jnp.where(even, weight, 0.0).astype(BF16), jnp.where(even, 0.0, weight).astype(BF16)
        ]
        summed = sum(
            jnp.dot(
                split[b][:, e * span : (e + 1) * span], values[e, b, :, at],
                preferred_element_type=F32,
            )
            for b in range(prompts)
            for e in range(CORES)
        )
        some = total > 0.0
        total = jnp.where(some, total, 1.0)
        level = jnp.broadcast_to(
            jnp.where(some, top + jnp.log(total), MASKED), (lines, LANES)
        )
        summed = summed / total
        for r in range(group):
            own = slice(r * ROWS, (r + 1) * ROWS)
            cs[n, r] = packed(summed[own], level[own])
        across = lax.rem(g + GROUPS // 2, GROUPS)
        for r in range(group):
            p = (CHIPS // GROUPS) * across + HEAD_AT[r]

            def go(n=n, r=r, p=p):
                slot = lax.rem(chip - p + CHIPS, CHIPS) - 1
                send(cs.at[n, r], cr.at[slot], ssem.at[8], rsem.at[8], p * CORES + c)

            if n < GROUPS - 1:
                go()
            else:
                pl.when(within != HEAD_AT[r])(go)

    rc, c_on = position(within, HEAD_AT)
    gc = lax.rem(half_group + GROUPS // 2, GROUPS)
    hc = HALF_HEADS * c + group * gc + rc

    @pl.when(c_on)
    def _():
        base = UNITS * gc
        query = jflat[:, lanes_of(base + rc)]
        new_key = jflat[:, lanes_of(base + group)]
        new_value = jflat[:, lanes_of(base + group + 1)]
        small_r = lax.broadcasted_iota(jnp.int32, (ROWS, ROWS), 0)
        small_c = lax.broadcasted_iota(jnp.int32, (ROWS, ROWS), 1)
        seen = jnp.logical_and(
            small_c <= small_r, lax.rem(small_c, prompts) == lax.rem(small_r, prompts)
        )
        score = lax.dot_general(query, new_key, nt, preferred_element_type=F32) * score_scale
        score = jnp.where(seen, score, MASKED)
        top = jnp.max(score, axis=-1, keepdims=True)
        weight = jnp.where(seen, jnp.exp(score - top), 0.0)
        total = jnp.sum(weight, axis=-1, keepdims=True)
        new_sum = jnp.dot(weight.astype(BF16), new_value, preferred_element_type=F32)
        best = top + jnp.log(total)
        levels[CHIPS] = jnp.broadcast_to(best, (ROWS, LANES))
        best = levels[CHIPS]
        wait_bytes(cr, rsem.at[8])

        def partial(s):
            return cs[GROUPS - 1, rc] if s == CHIPS - 1 else cr[s]

        for s in range(CHIPS):
            level = join_level(partial(s)[ROWS:].astype(F32))
            levels[s] = level
            best = jnp.maximum(best, level)
        den = jnp.exp(levels[CHIPS] - best)
        acc = new_sum / total * den
        for s in range(CHIPS):
            scale = jnp.exp(levels[s] - best)
            acc = acc + partial(s)[:ROWS].astype(F32) * scale
            den = den + scale
        aflat[:, lanes_of(hc)] = (acc / den).astype(BF16)
        to_all(aflat.at[:, lanes_of(hc)], ssem.at[9], rsem.at[9])
        wait_bytes(aflat.at[:, : (HEADS - 1) * LANES], rsem.at[9])

    @pl.when(jnp.logical_not(c_on))
    def _():
        wait_bytes(aflat, rsem.at[9])

    weights[5].wait()
    swaps[5].wait_recv()
    attended = aflat[...]
    tmp[...] = jnp.zeros((ROWS, LANES), F32)
    for e in range(CORES):
        tmp[:, e * width : (e + 1) * width] = lax.dot_general(
            attended, wout[e], nt, preferred_element_type=F32
        )
    mid = jnp.where(lane < pair, tmp[...] + stream, 0.0)
    mb[chip] = mid.astype(BF16)
    to_core(mb.at[chip], ssem.at[11], rsem.at[11])

    att_ref[...] = attended
    for w in weights[6:]:
        w.wait()
    wait_bytes(mb.at[pl.ds(0, CHIPS - 1)], rsem.at[11])
    mids = join_pieces([mb[p].astype(F32) for p in range(CHIPS)], pair, XS * tiles)
    square = jnp.zeros((ROWS, LANES), F32)
    for v in mids:
        square = square + v * v
    scale = lax.rsqrt(jnp.sum(square, axis=-1, keepdims=True) / (XS * block) + NORM_EPS)
    gain = mgain_ref[...].astype(F32)
    for g, v in enumerate(mids):
        nflat[:, g * LANES : (g + 1) * LANES] = (v * scale * gain[g : g + 1, :]).astype(BF16)
    normed_mid = nflat[...]
    both = jnp.dot(normed_mid, wgu[...], preferred_element_type=F32)
    gate, upper = both[:, :LANES], both[:, LANES:]
    hidden = (gate / (1.0 + jnp.exp(-gate)) * upper).astype(BF16)
    for batch in (range(2), range(2, XS)):
        for k in batch:
            es[k] = jnp.dot(hidden, wdown[k], preferred_element_type=F32).astype(BF16)
        for k in batch:
            if k < XS - 1:
                d, p = x_peers[k]
                send(es.at[k], er.at[d - 1], ssem.at[12], rsem.at[12], p * PLANE + j0)
    wait_bytes(er, rsem.at[12])
    total = es[XS - 1].astype(F32)
    for k in range(XS - 1):
        total = total + er[k].astype(F32)
    found = [total[:, t * LANES : (t + 1) * LANES] for t in range(tiles)]
    for j, piece in enumerate(cut_pieces(found, width, PLANE)):
        e2s[j] = piece.astype(BF16)
    for k, e, p in plane_peers:
        send(e2s.at[p], e2r.at[k * CORES + e - 1], ssem.at[13], rsem.at[13], x * PLANE + p)
    wait_bytes(e2r, rsem.at[13])
    final = e2s[j0].astype(F32)
    for k in range(PLANE - 1):
        final = final + e2r[k].astype(F32)
    final = final + jnp.where(row * 0 + c == 0, mid, pltpu.roll(mid, LANES - width, 1))
    lay_ref[...] = final[:, :width].astype(BF16)

    for sem, ref in (
        (0, a1r), (2, a2r), (12, er), (13, e2r),
    ):
        wait_bytes(ref, ssem.at[sem])
    wait_bytes(mb.at[pl.ds(0, CHIPS - 1)], ssem.at[11])
    for w in swaps:
        w.wait_send()

    @pl.when(b_on)
    def _():
        wait_bytes(br.at[pl.ds(0, HALF_JOINT - 1)], ssem.at[5])
        wait_bytes(mb.at[pl.ds(0, CHIPS - 1)], ssem.at[6])

    @pl.when(jnp.logical_not(b_on))
    def _():
        wait_bytes(br.at[pl.ds(0, HALF_JOINT)], ssem.at[5])

    @pl.when(c_on)
    def _():
        wait_bytes(cr.at[pl.ds(0, HALF_HEADS - 1)], ssem.at[8])
        wait_bytes(dummy, ssem.at[9])

    @pl.when(jnp.logical_not(c_on))
    def _():
        wait_bytes(cr.at[pl.ds(0, HALF_HEADS)], ssem.at[8])


def body(
    token_ids, lengths, embed_table, attn_gain, w_qkv, qkv_bias, cache_keys, cache_values, w_out,
    mlp_gain, w_gate, w_up, w_down,
):
    steps, prompts = token_ids.shape
    vocab_rows, model = embed_table.shape
    span = cache_keys.shape[1]
    width = w_out.shape[1]
    block = PLANE * width
    per_group = HEADS // KV_HEADS
    half = HEAD_DIM // 2
    frequency = np.float32(ROPE_BASE) ** (
        np.float32(-2.0) * np.arange(half, dtype=np.float32) / np.float32(HEAD_DIM)
    )
    frequency = jnp.asarray(np.tile(np.concatenate([frequency, frequency]), (ROWS, 1)), F32)
    vmem = pl.BlockSpec(memory_space=pltpu.VMEM)
    smem = pl.BlockSpec(memory_space=pltpu.SMEM)
    hbm = pl.BlockSpec(memory_space=pl.ANY)
    w_out_t = w_out.T

    def like(a):
        return pltpu.VMEM(a.shape, a.dtype)

    def tile(*lead, dtype=F32):
        return pltpu.VMEM((*lead, ROWS, LANES), dtype)

    def wide(*lead, dtype):
        return pltpu.VMEM((*lead, ROWS, block), dtype)

    def wider(*lead):
        return pltpu.VMEM((*lead, ROWS, block + LANES), BF16)

    attended, layer_out = pl.pallas_call(
        kernel,
        out_shape=(
            pltpu.VMEM((ROWS, HEADS * HEAD_DIM), BF16),
            pltpu.VMEM((ROWS, width), BF16),
        ),
        in_specs=[smem, smem, vmem, hbm, vmem, hbm, vmem, hbm, hbm, hbm, vmem, hbm, hbm, hbm],
        out_specs=(vmem, vmem),
        scratch_shapes=[
            pltpu.VMEM((XS, vocab_rows, block), BF16),
            pltpu.VMEM((CORES, width, HALF_JOINT * LANES), BF16),
            pltpu.VMEM((CORES, prompts, span, GROUPS * LANES), BF16),
            pltpu.VMEM((CORES, prompts, span, GROUPS * LANES), BF16),
            pltpu.VMEM((CORES, width, model), BF16),
            pltpu.VMEM((model, 2 * LANES), BF16), pltpu.VMEM((XS, LANES, block), BF16),
            wider(XS), wider(XS - 1),
            tile(YS), tile(PLANE - 1), tile(), tile(),
            tile(GROUPS, UNITS), tile(CHIPS - 1),
            pltpu.VMEM((ROWS, HALF_JOINT * LANES), BF16),
            pltpu.VMEM((GROUPS, per_group, 2 * ROWS, LANES), BF16),
            pltpu.VMEM((CHIPS - 1, 2 * ROWS, LANES), BF16), tile(CHIPS + 1),
            pltpu.VMEM((ROWS, HEADS * LANES), BF16),
            tile(), tile(CHIPS, dtype=BF16),
            pltpu.VMEM((ROWS, model), BF16),
            wide(XS, dtype=BF16), wide(XS - 1, dtype=BF16),
            tile(PLANE, dtype=BF16), tile(PLANE - 1, dtype=BF16),
            tile(GROUP - 1, dtype=BF16),
            pltpu.SemaphoreType.DMA((XS,)),
            pltpu.SemaphoreType.DMA((8 + XS,)),
            pltpu.SemaphoreType.DMA((14,)),
            pltpu.SemaphoreType.DMA((14,)),
            pltpu.SemaphoreType.DMA((GROUPS,)),
            pltpu.SemaphoreType.DMA((6,)),
            pltpu.SemaphoreType.DMA((6,)),
        ],
        compiler_params=pltpu.CompilerParams(
            collective_id=0, has_side_effects=True, vmem_limit_bytes=60 * 2**20
        ),
        name="layer",
    )(
        token_ids.T, lengths, frequency, embed_table, attn_gain.reshape(-1, LANES), w_qkv,
        qkv_bias.reshape(-1, LANES), cache_keys, cache_values, w_out_t,
        mlp_gain.reshape(-1, LANES), w_gate, w_up, w_down,
    )
    return pl.pallas_call(
        finish,
        out_shape=(
            jax.ShapeDtypeStruct((steps, prompts, HEADS * HEAD_DIM), BF16),
            jax.ShapeDtypeStruct((steps, prompts, width), BF16),
        ),
        in_specs=[vmem, vmem],
        out_specs=(vmem, vmem),
        name="finish",
    )(
        pltpu.with_memory_space_constraint(attended, pltpu.VMEM),
        pltpu.with_memory_space_constraint(layer_out, pltpu.VMEM),
    )


def finish(att_ref, lay_ref, att_out, lay_out):
    n = att_out.shape[1]
    for k in range(att_out.shape[0]):
        att_out[k] = att_ref[k * n : (k + 1) * n]
        lay_out[k] = lay_ref[k * n : (k + 1) * n]


def solution(mesh):
    return jax.shard_map(
        body,
        mesh=mesh,
        in_specs=(
            P(None, "parts"), P("parts"), P("seq", None), P(), P("seq", None), P(),
            P("parts", "seq", None), P("parts", "seq", None), P(None, "seq"), P(),
            P(None, "seq"), P(None, "seq"), P("seq", None),
        ),
        out_specs=(P(None, "parts", None), P(None, "parts", "seq")),
        check_vma=False,
    )
```
